128 devices in a mesh: rep: 1, dp: 128 (over x, y, z, core).
Axes of the slice: x: 4, y: 4, z: 4, core: 2. Of those that a mesh axis runs over, the one named last changes fastest.
Arguments:
- x: bfloat16 [128, 1024, 512], P(('rep', 'dp'))
- dy: bfloat16 [128, 1024, 512], P(('rep', 'dp'))
- w_gate: bfloat16 [2, 512, 4096], replicated
- w_up: bfloat16 [2, 512, 4096], replicated
- w_down: bfloat16 [2, 4096, 512], replicated
- m_w_gate: float32 [2, 512, 4096], replicated
- m_w_up: float32 [2, 512, 4096], replicated
- m_w_down: float32 [2, 4096, 512], replicated
- v_w_gate: float32 [2, 512, 4096], replicated
- v_w_up: float32 [2, 512, 4096], replicated
- v_w_down: float32 [2, 4096, 512], replicated
Outputs:
- output 1: bfloat16 [2, 512, 4096], P('rep')
- output 2: bfloat16 [2, 512, 4096], P('rep')
- output 3: bfloat16 [2, 4096, 512], P('rep')
- output 4: float32 [2, 512, 4096], P('rep')
- output 5: float32 [2, 512, 4096], P('rep')
- output 6: float32 [2, 4096, 512], P('rep')
- output 7: float32 [2, 512, 4096], P('rep')
- output 8: float32 [2, 512, 4096], P('rep')
- output 9: float32 [2, 4096, 512], P('rep')
All inputs are finite; a program needn't handle non-finite values.
Results may differ from the reference program's by a relative error of at most 0.022.
Values are sent between devices in bfloat16 or wider.
A program may use at most 1.5 GiB of HBM per device.

```python
import jax
import jax.numpy as jnp
from jax import lax

SEQUENCES = 128
TOKENS = 1024
D = 512
FF = 4096
LAYERS = 2
NAMES = ("w_gate", "w_up", "w_down")
SHAPES = {"w_gate": (LAYERS, D, FF), "w_up": (LAYERS, D, FF), "w_down": (LAYERS, FF, D)}


def bump(key, n, height):
    away = (jnp.arange(n, dtype=jnp.int32) - jax.random.randint(key, (), 0, n, jnp.int32)) % n
    return jnp.where(away < n // 8, height, 1.0)


def together(key, own, strength):
    shared = jax.random.normal(key, own.shape[1:], jnp.float32)
    return (own + strength * shared) * lax.rsqrt(1 + strength * strength)


def setup_inputs(seed: int = 0, part: int = 0) -> dict:
    kx, kdy, ka, kb, kz, kf, kh, kl, *keys = jax.random.split(jax.random.key(seed), 8 + 3 * len(NAMES))
    kx, kdy, ka, kb = (jax.random.fold_in(k, part) for k in (kx, kdy, ka, kb))
    kw, km, kv = (keys[i::3] for i in range(3))
    shape = (SEQUENCES, TOKENS, D)
    much_x, much_dy = jax.random.uniform(kz, (2,), jnp.float32, 0.0, 1.0)
    loud = 2.0 ** jax.random.uniform(jax.random.fold_in(kz, 1), (), jnp.float32, -1.0, 2.0)
    layers = 2.0 ** jax.random.uniform(kl, (LAYERS, 1, 1), jnp.float32, -1.0, 1.0)
    x = together(ka, jax.random.normal(kx, shape, jnp.float32), much_x) * bump(kf, D, 4.0)
    dy = together(kb, jax.random.normal(kdy, shape, jnp.float32), much_dy)
    drawn = {"x": x.astype(jnp.bfloat16), "dy": (loud * dy * (SEQUENCES * TOKENS) ** -0.5).astype(jnp.bfloat16)}
    for key, name in zip(kw, NAMES, strict=True):
        w = jax.random.normal(key, SHAPES[name], jnp.float32) * SHAPES[name][1] ** -0.5
        drawn[name] = (w * {"w_gate": 1.0, "w_up": bump(kh, FF, 4.0), "w_down": layers}[name]).astype(jnp.bfloat16)
    for key, name in zip(km, NAMES, strict=True):
        drawn[f"m_{name}"] = 0.1 * jax.random.normal(key, SHAPES[name], jnp.float32)
    for key, name in zip(kv, NAMES, strict=True):
        drawn[f"v_{name}"] = jax.random.uniform(key, SHAPES[name], jnp.float32, 0.005, 0.015)
    return drawn


def matmul(a, w):
    return jnp.dot(a, w, preferred_element_type=jnp.float32).astype(jnp.bfloat16)


def normed(h):
    wide = h.astype(jnp.float32)
    scale = lax.rsqrt(jnp.mean(wide**2, -1, keepdims=True) + 1e-6)
    return (wide * scale).astype(jnp.bfloat16)


def layer(h, w):
    a = normed(h)
    gate = jnp.dot(a, w["w_gate"], preferred_element_type=jnp.float32)
    up = jnp.dot(a, w["w_up"], preferred_element_type=jnp.float32)
    return h + matmul((jax.nn.silu(gate) * up).astype(jnp.bfloat16), w["w_down"])


def adamw(w, m, v, g):
    m = 0.9 * m + 0.1 * g
    v = 0.95 * v + 0.05 * g * g
    step = m * lax.rsqrt(v + 1e-8) + 0.1 * w
    return (w - 0.02 * step).astype(jnp.bfloat16), m, v


def clipped(gradients, sum_of_squares, count):
    factor = jnp.minimum(1.0, 0.5 * lax.rsqrt(sum_of_squares / count + 1e-30))
    return [g * factor for g in gradients]


def stack(weights, h):
    return lax.scan(lambda h, w: (layer(h, w), None), h, weights)[0]


def reference(x, dy, w_gate, w_up, w_down, m_w_gate, m_w_up, m_w_down, v_w_gate, v_w_up, v_w_down):
    weights = dict(zip(NAMES, (w_gate, w_up, w_down), strict=True))

    def take(so_far, sequence):
        h, by_y = sequence
        _, back = jax.vjp(lambda w: stack(w, h), weights)
        return jax.tree.map(lambda total, term: total + term.astype(jnp.float32), so_far, back(by_y)[0]), None

    none_yet = {name: jnp.zeros(w.shape, jnp.float32) for name, w in weights.items()}
    by_weights, _ = lax.scan(take, none_yet, (x, dy))
    gradients = [by_weights[name].astype(jnp.bfloat16).astype(jnp.float32) for name in NAMES]
    gradients = clipped(gradients, sum(jnp.sum(g * g) for g in gradients), sum(g.size for g in gradients))
    new = [
        adamw(w.astype(jnp.float32), m, v, g)
        for w, m, v, g in zip((w_gate, w_up, w_down), (m_w_gate, m_w_up, m_w_down), (v_w_gate, v_w_up, v_w_down), gradients, strict=True)
    ]
    return tuple(one[which] for which in range(3) for one in new)
```

```python
import functools

import jax
import jax.numpy as jnp
from jax import lax
from jax.experimental import pallas as pl
from jax.experimental.pallas import tpu as pltpu
from jax.sharding import PartitionSpec as P

NAMES = ("w_gate", "w_up", "w_down")
COUNT = 2 * 3 * 512 * 4096
F32, BF16 = jnp.float32, jnp.bfloat16
STRIDE = (32, 8, 2)


def matmul(a, w):
    return jnp.dot(a, w, preferred_element_type=jnp.float32).astype(jnp.bfloat16)


def normed(h):
    wide = h.astype(jnp.float32)
    scale = lax.rsqrt(jnp.mean(wide**2, -1, keepdims=True) + 1e-6)
    return (wide * scale).astype(jnp.bfloat16)


def layer(h, w):
    a = normed(h)
    gate = jnp.dot(a, w["w_gate"], preferred_element_type=jnp.float32)
    up = jnp.dot(a, w["w_up"], preferred_element_type=jnp.float32)
    return h + matmul((jax.nn.silu(gate) * up).astype(jnp.bfloat16), w["w_down"])


def place():
    me = lax.axis_index("dp")
    return me, lax.rem(me, 2), [lax.rem(lax.div(me, s), 4) for s in STRIDE]


def neighbour(me, p, d, by):
    return me + (lax.rem(p[d] + by, 4) - p[d]) * STRIDE[d]


HALF, SIZES = 2048, (512, 128, 32)


def reduce_kernel(g00, g01, g10, g11, g20, g21, c0, c1, c2, factor, H, R0, R1, R2, R3, F1, F2, C, N, sq,
                  lsem, ds, dr, ps, pr, gs, gr, ns, nr, osem):
    g, outs = ((g00, g01), (g10, g11), (g20, g21)), (c0, c1, c2)
    me, core, p = place()
    partner = me + 1 - 2 * core
    dims = [(c, (c + 1) % 3, (c + 2) % 3) for c in range(3)]

    def send(src, dst, s, r, to):
        copy = pltpu.make_async_remote_copy(src_ref=src, dst_ref=dst, send_sem=s, recv_sem=r, device_id={"dp": to}, device_id_type=pl.DeviceIdType.MESH)
        copy.start()
        return copy

    barrier = pltpu.get_barrier_semaphore()
    others = [partner] + [neighbour(me, p, d, by) for d in range(3) for by in (1, 2, 3)]
    for other in others:
        pl.semaphore_signal(barrier, inc=1, device_id={"dp": other}, device_id_type=pl.DeviceIdType.MESH)

    loads = [pltpu.make_async_copy(g[c][l].at[pl.ds(pl.multiple_of(core * HALF, HALF), HALF)], H.at[c, l], lsem.at[c, l]) for c in range(3) for l in range(2)]
    for load in loads:
        load.start()
    pl.semaphore_wait(barrier, len(others))

    swaps = {}
    for by in (2, 3, 1, 0):
        for c in range(3):
            for l in range(2):
                at = pl.multiple_of(lax.rem(p[c] + by, 4) * 512, 512)
                swaps[c, by, l] = send(g[c][l].at[pl.ds(pl.multiple_of((1 - core) * HALF, HALF) + at, 512)], R0.at[c, l, pl.ds(at, 512)], ds.at[c, by, l], dr.at[c, by, l], partner)
    for load in loads:
        load.wait()

    sends = []

    def stage(k):
        size, R = SIZES[k], (R1, R2, R3)[k]
        half = size // 2
        step = min(half, 32)

        def begin(c):
            return sum((p[dims[c][i]] * SIZES[i] for i in range(k)), jnp.int32(0))

        def term(c, l, at, row):
            if k == 0:
                rows = pl.ds(pl.multiple_of(at + row, 16), step)
                return H[c, l, rows].astype(F32) + R0[c, l, rows].astype(F32)
            return (F1, F2)[k - 1][c, l, pl.ds(pl.multiple_of(at + row, 16), step)]

        def make(c, at, slots, keep):
            for l in range(2):
                def body(i, carry):
                    row = pl.multiple_of(i * step, 16)
                    total = term(c, l, at, row)
                    for slot in slots:
                        total += R[c, slot, l, pl.ds(row, step)].astype(F32)
                    keep(l, row, total)
                    return carry
                lax.fori_loop(0, half // step, body, 0)

        def leave(c, by, side, slots, to, slot):
            at = pl.multiple_of(lax.rem(p[dims[c][k]] + by, 4) * size + side * half, 16)
            base = pl.multiple_of(begin(c) + at, 16)

            def keep(l, row, total):
                H[c, l, pl.ds(pl.multiple_of(base + row, 16), step)] = total.astype(BF16)

            make(c, at, slots, keep)
            sends.append(send(H.at[c, :, pl.ds(base, half)], R.at[c, slot], ps.at[k, c, slot], pr.at[k, c, slot], neighbour(me, p, dims[c][k], to)))

        def arrived(c, slot):
            pltpu.make_async_copy(R.at[c, slot], R.at[c, slot], pr.at[k, c, slot]).wait()

        for c in range(3):
            if k == 0:
                swaps[c, 2, 0].wait_recv(), swaps[c, 2, 1].wait_recv()
            leave(c, 2, 0, (), 3, 0)
            leave(c, 2, 1, (), 1, 3)
        for c in range(3):
            if k == 0:
                for l in range(2):
                    swaps[c, 3, l].wait_recv(), swaps[c, 1, l].wait_recv()
            leave(c, 3, 1, (), 3, 1)
            leave(c, 1, 0, (), 1, 4)
        for c in range(3):
            arrived(c, 0)
            leave(c, 3, 0, (0,), 3, 2)
            arrived(c, 3)
            leave(c, 1, 1, (3,), 1, 5)
        for c in range(3):
            if k == 0:
                swaps[c, 0, 0].wait_recv(), swaps[c, 0, 1].wait_recv()
            for slot in (1, 4, 2, 5):
                arrived(c, slot)
            for side, slots in ((0, (2, 4)), (1, (1, 5))):
                at = pl.multiple_of(p[dims[c][k]] * size + side * half, 16)

                def keep(l, row, total):
                    if k < 2:
                        (F1, F2)[k][c, l, pl.ds(pl.multiple_of(side * half + row, 16), step)] = total
                    else:
                        rounded = total.astype(BF16)
                        C[c, l, pl.ds(pl.multiple_of(p[dims[c][1]] * 128 + p[dims[c][2]] * 32 + side * half, 16), step)] = rounded
                        wide = rounded.astype(F32)
                        wide = wide * wide
                        sq[...] += sum(wide[8 * a : 8 * a + 8, 128 * b : 128 * b + 128] for a in range(step // 8) for b in range(4))

                make(c, at, slots, keep)

    sq[...] = jnp.zeros_like(sq)
    stage(0)
    stage(1)
    stage(2)

    def square(n):
        to = [(partner, core, core)] if n == 0 else [(neighbour(me, p, n - 1, by), p[n - 1], by - 1) for by in (1, 2, 3)]
        mine = core if n == 0 else p[n - 1]
        N[n, mine] = sq[...]
        copies = []
        for i, (dev, _, _) in enumerate(to):
            copies.append(send(sq, N.at[n, mine], ns.at[n, i], nr.at[n, i], dev))
        return copies

    def squared(n, copies):
        for copy in copies:
            copy.wait()
        sq[...] = N[n, 0] + N[n, 1] if n == 0 else (N[n, 0] + N[n, 1]) + (N[n, 2] + N[n, 3])

    def rows(c, k, by):
        at = lax.rem(p[dims[c][k]] + by, 4) * SIZES[k]
        return pl.ds(pl.multiple_of(at + (p[dims[c][1]] * 128 if k == 2 else 0), 32), SIZES[k])

    def spread(k, c):
        own = C.at[c, :, rows(c, k, 0)]
        return [send(own, own, gs.at[k - 1, c, i], gr.at[k - 1, c, i], neighbour(me, p, dims[c][k], to)) for i, to in ((0, 3), (1, 1))]

    def relay(k, c, copies):
        more = []
        for i, by, to in ((0, 1, 3), (1, 3, 1)):
            whole = C.at[c, :, rows(c, k, by)]
            pltpu.make_async_copy(whole, whole, gr.at[k - 1, c, i]).wait()
            part = C.at[c, i, rows(c, k, by)]
            more.append(send(part, part, gs.at[k - 1, c, 2 + i], gr.at[k - 1, c, 2 + i], neighbour(me, p, dims[c][k], to)))
        return copies, more

    def gathered(k, c, copies, more):
        for i in range(2):
            part = C.at[c, i, rows(c, k, 2)]
            pltpu.make_async_copy(part, part, gr.at[k - 1, c, 2 + i]).wait()
        for copy in copies + more:
            copy.wait_send()

    copies = square(0)
    own = [spread(2, c) for c in range(3)]
    squared(0, copies)
    copies = square(1)
    more = [relay(2, c, own[c]) for c in range(3)]
    squared(1, copies)
    copies = square(2)
    for c in range(3):
        gathered(2, c, *more[c])
    own = [spread(1, c) for c in range(3)]
    squared(2, copies)
    copies = square(3)
    more = [relay(1, c, own[c]) for c in range(3)]
    squared(3, copies)
    factor[...] = jnp.full(factor.shape, jnp.minimum(1.0, 0.5 * lax.rsqrt(jnp.sum(sq[...], keepdims=True) / COUNT + 1e-30)), F32)
    stores = []
    for c in range(3):
        gathered(1, c, *more[c])
        stores.append(pltpu.make_async_copy(C.at[c], outs[c], osem.at[c]))
        stores[-1].start()
    for copy in list(swaps.values()) + sends:
        copy.wait_send()
    for store in stores:
        store.wait()


def reduce_all(g):
    dma, vmem = pltpu.SemaphoreType.DMA, pltpu.VMEM
    hbm = pl.BlockSpec(memory_space=pl.ANY)
    return pl.pallas_call(
        reduce_kernel,
        out_shape=[jax.ShapeDtypeStruct((2, 512, 512), BF16)] * 3 + [jax.ShapeDtypeStruct((8, 128), F32)],
        in_specs=[hbm] * 6,
        out_specs=[hbm] * 3 + [pl.BlockSpec(memory_space=pltpu.VMEM)],
        scratch_shapes=[
            vmem((3, 2, HALF, 512), BF16),
            vmem((3, 2, HALF, 512), BF16),
            vmem((3, 6, 2, 256, 512), BF16),
            vmem((3, 6, 2, 64, 512), BF16),
            vmem((3, 6, 2, 16, 512), BF16),
            vmem((3, 2, 512, 512), F32),
            vmem((3, 2, 128, 512), F32),
            vmem((3, 2, 512, 512), BF16),
            vmem((4, 4, 8, 128), F32),
            vmem((8, 128), F32),
            dma((3, 2)),
            dma((3, 4, 2)), dma((3, 4, 2)),
            dma((3, 3, 6)), dma((3, 3, 6)),
            dma((2, 3, 4)), dma((2, 3, 4)),
            dma((4, 3)), dma((4, 3)),
            dma((3,)),
        ],
        compiler_params=pltpu.CompilerParams(collective_id=1, has_side_effects=True, vmem_limit_bytes=60 * 2**20),
        name="reduce_all",
    )(*g)


def adamw_kernel(n_g, first, meta, f, *refs):
    unit = pl.program_id(0)
    ins, refs = refs[:9], refs[9:]
    g, refs = refs[: 3 * n_g], refs[3 * n_g :]
    outs = refs if first else refs[9:]
    outs[9][...] = jnp.zeros_like(outs[9])
    factor = f[0, 0]

    def update(c, gref, shape_of):
        w, m, v = ins[c], ins[3 + c], ins[6 + c]
        ow, om, ov = outs[c], outs[3 + c], outs[6 + c]

        def body(i, carry):
            if c < 2:
                at = (0, pl.ds(0, 32), pl.ds(pl.multiple_of(i * 512, 512), 512))
                wide = gref[0, i].astype(F32) * factor
            else:
                at = (0, pl.ds(pl.multiple_of(i * 32, 32), 32), slice(None))
                wide = gref[0, i].astype(F32) * factor
            nm = 0.9 * m[at] + 0.1 * wide
            nv = 0.95 * v[at] + 0.05 * wide * wide
            old = w[at].astype(F32)
            om[at] = nm
            ov[at] = nv
            ow[at] = (old - 0.02 * (nm * lax.rsqrt(nv + 1e-8) + 0.1 * old)).astype(BF16)
            return carry

        lax.fori_loop(0, 8, body, 0, unroll=2)

    for k in range(n_g):
        @pl.when(unit == k)
        def _():
            for c in range(3):
                update(c, g[3 * k + c], None)


def adamw_part(units, f, state, so_far):
    n_g = len(units)
    meta = jnp.stack([jnp.stack([*q, jnp.int32(l)]).astype(jnp.int32) for q, l, _, _ in units])

    def rows(c):
        return lambda u, i, meta: (meta[u, 3], meta[u, c] * 2 + i, 0)

    wide, tall = (1, 32, 4096), (1, 256, 512)
    state_specs = [pl.BlockSpec(tall if c == 2 else wide, rows(c)) for _ in range(3) for c in range(3)]

    def part(k, index):
        return pl.BlockSpec((1, 8, 32, 512), lambda u, i, meta: (index, jnp.clip(u * 2 + i - 2 * k, 0, 1), 0, 0))

    grads, grad_specs = [], []
    for k, (_, _, arrays, index) in enumerate(units):
        for c in range(3):
            grads.append(arrays[c].reshape(arrays[c].shape[0], 16, 32, 512))
            grad_specs.append(part(k, index))
    before = [] if so_far is None else list(so_far)
    shapes = [jax.ShapeDtypeStruct(a.shape, a.dtype) for a in state] + [jax.ShapeDtypeStruct((8, 128), F32)]
    elements = n_g * 3 * 262144
    return pl.pallas_call(
        functools.partial(adamw_kernel, n_g, so_far is None),
        out_shape=shapes,
        grid_spec=pltpu.PrefetchScalarGridSpec(
            num_scalar_prefetch=1,
            grid=(n_g, 2),
            in_specs=[pl.BlockSpec((8, 128), lambda u, i, meta: (0, 0), memory_space=pltpu.SMEM)] + state_specs + grad_specs + [pl.BlockSpec(memory_space=pl.ANY)] * len(before),
            out_specs=state_specs + [pl.BlockSpec((8, 128), lambda u, i, meta: (0, 0))],
        ),
        input_output_aliases={2 + 9 + 3 * n_g + i: i for i in range(len(before))},
        compiler_params=pltpu.CompilerParams(dimension_semantics=("arbitrary", "arbitrary"), vmem_limit_bytes=60 * 2**20),
        cost_estimate=pl.CostEstimate(flops=elements * 400, bytes_accessed=elements * 22, transcendentals=elements),
        name="adamw",
    )(meta, f, *state, *grads, *before)


def ring(d, by):
    return [(i, i + ((i // STRIDE[d] % 4 + by) % 4 - i // STRIDE[d] % 4) * STRIDE[d]) for i in range(128)]


PARTNER = [(i, i ^ 1) for i in range(128)]


def blocks(g, c):
    return g if c == 2 else g.reshape(16, 32, 8, 512).transpose(0, 2, 1, 3).reshape(4096, 512)


def finish(g, weights, m, v):
    c0, c1, c2, f = reduce_all([blocks(g[c][l], c) for c in range(3) for l in range(2)])
    own = (c0, c1, c2)

    def swap(arrays):
        return [lax.ppermute(a, "dp", PARTNER) for a in arrays]

    after = [lax.ppermute(own[c], "dp", ring(c, 3)) for c in range(3)]
    ahead = [lax.ppermute(own[c], "dp", ring(c, 1)) for c in range(3)]
    own_x = swap(own)

    me, core, p = place()

    def q(by, other):
        return [(1 - core if other else core) * 4 + lax.rem(p[c] + by, 4) for c in range(3)]

    def units(by, other, arrays):
        return [(q(by, other), l, arrays, l) for l in range(2)]

    def held(arrays, token):
        return [lax.optimization_barrier((a, token))[0] for a in arrays]

    state = [*weights, *m, *v]
    *so_far, token = adamw_part(units(0, 0, own), f, state, None)
    *so_far, token = adamw_part(units(0, 1, own_x), f, state, so_far)
    after_held, ahead_held = held(after, token), held(ahead, token)
    far = [lax.ppermute(after_held[c], "dp", ring(c, 3)) for c in range(3)]
    after_x, ahead_x = swap(after_held), swap(ahead_held)
    *so_far, token = adamw_part(units(1, 0, after) + units(3, 0, ahead), f, state, so_far)
    far_held = held(far, token)
    far_x = swap(far_held)
    *so_far, token = adamw_part(units(1, 1, after_x) + units(3, 1, ahead_x) + units(2, 0, far), f, state, so_far)
    *so_far, token = adamw_part(units(2, 1, far_x), f, state, so_far)
    return tuple(so_far)


def solution(mesh):
    def step(x, dy, *arrays):
        weights, m, v = (arrays[i : i + 3] for i in (0, 3, 6))
        layers = weights[0].shape[0]
        h, kept = x[0], []
        for number in range(layers):
            kept.append(h)
            h = layer(h, {name: w[number] for name, w in zip(NAMES, weights, strict=True)})
        by_h, terms = dy[0], [None] * layers
        for number in reversed(range(layers)):
            _, back = jax.vjp(lambda w, h: layer(h, w), {name: w[number] for name, w in zip(NAMES, weights, strict=True)}, kept[number])
            by_w, by_h = back(by_h)
            terms[number] = [by_w[name] for name in NAMES]
        return finish([[terms[l][c] for l in range(2)] for c in range(3)], weights, m, v)

    return jax.shard_map(
        step,
        mesh=mesh,
        in_specs=(P(("rep", "dp"), None, None),) * 2 + (P(None, None, None),) * 9,
        out_specs=(P("rep", None, None),) * 9,
        check_vma=False,
    )
```

```python
import functools

import jax
import jax.numpy as jnp
from jax import lax
from jax.experimental import pallas as pl
from jax.experimental.pallas import tpu as pltpu
from jax.sharding import PartitionSpec as P

COUNT = 2 * 3 * 512 * 4096
F32, BF16 = jnp.float32, jnp.bfloat16
STRIDE = (32, 8, 2)


ROWS, TILE, CHUNK, PIECE = 1024, 512, 256, 32


def dot(a, b, dims=((1,), (0,))):
    return lax.dot_general(a, b, (dims, ((), ())), preferred_element_type=F32)


def norm_into(h_ref, a, scale=None):
    for r in range(0, ROWS, 128):
        wide = h_ref[r : r + 128, :].astype(F32)
        by = lax.rsqrt(jnp.mean(wide * wide, -1, keepdims=True) + 1e-6)
        a[r : r + 128, :] = (wide * by).astype(BF16)
        if scale is not None:
            scale[r : r + 128, :] = jnp.broadcast_to(by, (128, 128))


def flip_into(a, t):
    for r in range(0, ROWS, 256):
        t[:, r : r + 256] = a[r : r + 256, :].T


def forward_kernel(x, wg, wu, wd, gate, up, h1, a, s, acc):
    j = pl.program_id(0)

    @pl.when(j == 0)
    def _():
        norm_into(x, a)
        acc[...] = jnp.zeros_like(acc)

    for r in range(0, ROWS, CHUNK):
        at = pl.ds(r, CHUNK)
        gate[at, :] = dot(a[at, :], wg[0])
        up[at, :] = dot(a[at, :], wu[0])
        for i in range(r, r + CHUNK, PIECE):
            g = gate[i : i + PIECE, :]
            s[i : i + PIECE, :] = (g * jax.nn.sigmoid(g) * up[i : i + PIECE, :]).astype(BF16)
        acc[at, :] += dot(s[at, :], wd[0])

    @pl.when(j == pl.num_programs(0) - 1)
    def _():
        for r in range(0, ROWS, 128):
            h1[r : r + 128, :] = x[r : r + 128, :] + acc[r : r + 128, :].astype(BF16)


def gated(g, u, d):
    sig = jax.nn.sigmoid(g)
    silu = g * sig
    d = d.astype(BF16).astype(F32)
    du = d * silu
    ds = d * u
    return (silu * u).astype(BF16), (ds * sig + ds * g * (sig * (1.0 - sig))).astype(BF16), du.astype(BF16)


def weight_gradients(at, yt, s, dg, du, og, ou, od):
    for half in range(2):
        rows = slice(half * 256, half * 256 + 256)
        og[half * 8 : half * 8 + 8, 0] = dot(at[rows, :], dg[...]).astype(BF16).reshape(8, 32, TILE)
        ou[half * 8 : half * 8 + 8, 0] = dot(at[rows, :], du[...]).astype(BF16).reshape(8, 32, TILE)
        od[:, rows] = dot(yt[rows, :], s[...]).astype(BF16).T


def last_kernel(h1, dy, wg, wu, wd, og, ou, od, dh, a, at, yt, s, dg, du, gate, up, ds, accg, accu, scale):
    j = pl.program_id(0)

    @pl.when(j == 0)
    def _():
        norm_into(h1, a, scale)
        flip_into(a, at)
        flip_into(dy, yt)
        accg[...] = jnp.zeros_like(accg)
        accu[...] = jnp.zeros_like(accu)

    for r in range(0, ROWS, CHUNK):
        rows = pl.ds(r, CHUNK)
        gate[rows, :] = dot(a[rows, :], wg[0])
        up[rows, :] = dot(a[rows, :], wu[0])
        ds[rows, :] = dot(dy[rows, :], wd[0], ((1,), (1,)))
        for i in range(r, r + CHUNK, PIECE):
            k = slice(i, i + PIECE)
            s[k, :], dg[k, :], du[k, :] = gated(gate[k, :], up[k, :], ds[k, :])
        accg[rows, :] += dot(dg[rows, :], wg[0], ((1,), (1,)))
        accu[rows, :] += dot(du[rows, :], wu[0], ((1,), (1,)))
    weight_gradients(at, yt, s, dg, du, og, ou, od)

    @pl.when(j == pl.num_programs(0) - 1)
    def _():
        for r in range(0, ROWS, 64):
            k = slice(r, r + 64)
            by_a = (accg[k, :].astype(BF16) + accu[k, :].astype(BF16)).astype(F32)
            wide = h1[k, :].astype(F32)
            by = scale[k, :1]
            by_scale = jnp.sum(by_a * wide, -1, keepdims=True)
            by_wide = by_a * by + wide * (by_scale * (by * by * by) * (-1.0 / 512))
            dh[k, :] = dy[k, :] + by_wide.astype(BF16)


def first_kernel(x, dy, wd, gate, up, og, ou, od, a, at, yt, s, dg, du, ds):
    j = pl.program_id(0)

    @pl.when(j == 0)
    def _():
        norm_into(x, a)
        flip_into(a, at)
        flip_into(dy, yt)

    for r in range(0, ROWS, CHUNK):
        rows = pl.ds(r, CHUNK)
        ds[rows, :] = dot(dy[rows, :], wd[0], ((1,), (1,)))
        for i in range(r, r + CHUNK, PIECE):
            k = slice(i, i + PIECE)
            s[k, :], dg[k, :], du[k, :] = gated(gate[k, :], up[k, :], ds[k, :])
    weight_gradients(at, yt, s, dg, du, og, ou, od)


def terms(x, dy, w_gate, w_up, w_down):
    vmem = pltpu.VMEM
    steps = 4096 // TILE
    full = pl.BlockSpec((ROWS, 512), lambda j: (0, 0))
    tile = pl.BlockSpec((ROWS, TILE), lambda j: (0, j))
    shape = jax.ShapeDtypeStruct
    states, wide = shape((ROWS, 512), BF16), shape((ROWS, 4096), F32)

    def weight(l):
        return [pl.BlockSpec((1, 512, TILE), lambda j: (l, 0, j))] * 2 + [pl.BlockSpec((1, TILE, 512), lambda j: (l, j, 0))]

    grads = [shape((16, 8, 32, TILE), BF16)] * 2 + [shape((4096, 512), BF16)]
    grad_specs = [pl.BlockSpec((16, 1, 32, TILE), lambda j: (0, j, 0, 0))] * 2 + [pl.BlockSpec((TILE, 512), lambda j: (j, 0))]
    b, t, f = vmem((ROWS, 512), BF16), vmem((512, ROWS), BF16), vmem((ROWS, 512), F32)

    def call(kernel, dots, name, out_shape, in_specs, out_specs, scratch, *args):
        return pl.pallas_call(
            kernel, out_shape=out_shape, grid=(steps,), in_specs=in_specs, out_specs=out_specs, scratch_shapes=scratch, name=name,
            compiler_params=pltpu.CompilerParams(dimension_semantics=("arbitrary",), vmem_limit_bytes=60 * 2**20),
            cost_estimate=pl.CostEstimate(flops=dots * 2 * 1024 * 512 * 4096, bytes_accessed=30 * 2**20, transcendentals=2**22),
        )(*args)

    gate, up, h1 = call(forward_kernel, 3, "forward", [wide, wide, states], [full] + weight(0), [tile, tile, full], [b, b, f], x, w_gate, w_up, w_down)
    g1 = call(last_kernel, 8, "last", grads + [states], [full, full] + weight(1), grad_specs + [full],
              [b, t, t, b, b, b, f, f, f, f, f, vmem((ROWS, 128), F32)], h1, dy, w_gate, w_up, w_down)
    *g1, dh = g1
    g0 = call(first_kernel, 4, "first", grads, [full, full, weight(0)[2], tile, tile], grad_specs, [b, t, t, b, b, b, f], x, dh, w_down, gate, up)
    return [[g[c].reshape(4096, 512) for g in (g0, g1)] for c in range(3)]


def place():
    me = lax.axis_index("dp")
    return me, lax.rem(me, 2), [lax.rem(lax.div(me, s), 4) for s in STRIDE]


def neighbour(me, p, d, by):
    return me + (lax.rem(p[d] + by, 4) - p[d]) * STRIDE[d]


HALF, SIZES = 2048, (512, 128, 32)


def reduce_kernel(g00, g01, g10, g11, g20, g21, c0, c1, c2, factor, H, R0, R1, R2, R3, F1, F2, C, N, sq,
                  lsem, ds, dr, ps, pr, gs, gr, ns, nr, osem):
    g, outs = ((g00, g01), (g10, g11), (g20, g21)), (c0, c1, c2)
    me, core, p = place()
    partner = me + 1 - 2 * core
    dims = [(c, (c + 1) % 3, (c + 2) % 3) for c in range(3)]

    def send(src, dst, s, r, to):
        copy = pltpu.make_async_remote_copy(src_ref=src, dst_ref=dst, send_sem=s, recv_sem=r, device_id={"dp": to}, device_id_type=pl.DeviceIdType.MESH)
        copy.start()
        return copy

    barrier = pltpu.get_barrier_semaphore()
    others = [partner] + [neighbour(me, p, d, by) for d in range(3) for by in (1, 2, 3)]
    for other in others:
        pl.semaphore_signal(barrier, inc=1, device_id={"dp": other}, device_id_type=pl.DeviceIdType.MESH)

    loads = [pltpu.make_async_copy(g[c][l].at[pl.ds(pl.multiple_of(core * HALF, HALF), HALF)], H.at[c, l], lsem.at[c, l]) for c in range(3) for l in range(2)]
    for load in loads:
        load.start()
    pl.semaphore_wait(barrier, len(others))

    swaps = {}
    for by in (2, 3, 1, 0):
        for c in range(3):
            for l in range(2):
                at = pl.multiple_of(lax.rem(p[c] + by, 4) * 512, 512)
                swaps[c, by, l] = send(g[c][l].at[pl.ds(pl.multiple_of((1 - core) * HALF, HALF) + at, 512)], R0.at[c, l, pl.ds(at, 512)], ds.at[c, by, l], dr.at[c, by, l], partner)
    for load in loads:
        load.wait()

    sends = []

    def stage(k):
        size, R = SIZES[k], (R1, R2, R3)[k]
        half = size // 2
        step = min(half, 32)

        def begin(c):
            return sum((p[dims[c][i]] * SIZES[i] for i in range(k)), jnp.int32(0))

        def term(c, l, at, row):
            if k == 0:
                rows = pl.ds(pl.multiple_of(at + row, 16), step)
                return H[c, l, rows].astype(F32) + R0[c, l, rows].astype(F32)
            return (F1, F2)[k - 1][c, l, pl.ds(pl.multiple_of(at + row, 16), step)]

        def make(c, at, slots, keep):
            for l in range(2):
                def body(i, carry):
                    row = pl.multiple_of(i * step, 16)
                    total = term(c, l, at, row)
                    for slot in slots:
                        total += R[c, slot, l, pl.ds(row, step)].astype(F32)
                    keep(l, row, total)
                    return carry
                lax.fori_loop(0, half // step, body, 0)

        def leave(c, by, side, slots, to, slot):
            at = pl.multiple_of(lax.rem(p[dims[c][k]] + by, 4) * size + side * half, 16)
            base = pl.multiple_of(begin(c) + at, 16)

            def keep(l, row, total):
                H[c, l, pl.ds(pl.multiple_of(base + row, 16), step)] = total.astype(BF16)

            make(c, at, slots, keep)
            sends.append(send(H.at[c, :, pl.ds(base, half)], R.at[c, slot], ps.at[k, c, slot], pr.at[k, c, slot], neighbour(me, p, dims[c][k], to)))

        def arrived(c, slot):
            pltpu.make_async_copy(R.at[c, slot], R.at[c, slot], pr.at[k, c, slot]).wait()

        for c in range(3):
            if k == 0:
                swaps[c, 2, 0].wait_recv(), swaps[c, 2, 1].wait_recv()
            leave(c, 2, 0, (), 3, 0)
            leave(c, 2, 1, (), 1, 3)
        for c in range(3):
            if k == 0:
                for l in range(2):
                    swaps[c, 3, l].wait_recv(), swaps[c, 1, l].wait_recv()
            leave(c, 3, 1, (), 3, 1)
            leave(c, 1, 0, (), 1, 4)
        for c in range(3):
            arrived(c, 0)
            leave(c, 3, 0, (0,), 3, 2)
            arrived(c, 3)
            leave(c, 1, 1, (3,), 1, 5)
        for c in range(3):
            if k == 0:
                swaps[c, 0, 0].wait_recv(), swaps[c, 0, 1].wait_recv()
            for slot in (1, 4, 2, 5):
                arrived(c, slot)
            for side, slots in ((0, (2, 4)), (1, (1, 5))):
                at = pl.multiple_of(p[dims[c][k]] * size + side * half, 16)

                def keep(l, row, total):
                    if k < 2:
                        (F1, F2)[k][c, l, pl.ds(pl.multiple_of(side * half + row, 16), step)] = total
                    else:
                        rounded = total.astype(BF16)
                        C[c, l, pl.ds(pl.multiple_of(p[dims[c][1]] * 128 + p[dims[c][2]] * 32 + side * half, 16), step)] = rounded
                        wide = rounded.astype(F32)
                        wide = wide * wide
                        sq[...] += sum(wide[8 * a : 8 * a + 8, 128 * b : 128 * b + 128] for a in range(step // 8) for b in range(4))

                make(c, at, slots, keep)

    sq[...] = jnp.zeros_like(sq)
    stage(0)
    stage(1)
    stage(2)

    def square(n):
        to = [(partner, core, core)] if n == 0 else [(neighbour(me, p, n - 1, by), p[n - 1], by - 1) for by in (1, 2, 3)]
        mine = core if n == 0 else p[n - 1]
        N[n, mine] = sq[...]
        copies = []
        for i, (dev, _, _) in enumerate(to):
            copies.append(send(sq, N.at[n, mine], ns.at[n, i], nr.at[n, i], dev))
        return copies

    def squared(n, copies):
        for copy in copies:
            copy.wait()
        sq[...] = N[n, 0] + N[n, 1] if n == 0 else (N[n, 0] + N[n, 1]) + (N[n, 2] + N[n, 3])

    def rows(c, k, by):
        at = lax.rem(p[dims[c][k]] + by, 4) * SIZES[k]
        return pl.ds(pl.multiple_of(at + (p[dims[c][1]] * 128 if k == 2 else 0), 32), SIZES[k])

    def spread(k, c):
        own = C.at[c, :, rows(c, k, 0)]
        return [send(own, own, gs.at[k - 1, c, i], gr.at[k - 1, c, i], neighbour(me, p, dims[c][k], to)) for i, to in ((0, 3), (1, 1))]

    def relay(k, c, copies):
        more = []
        for i, by, to in ((0, 1, 3), (1, 3, 1)):
            whole = C.at[c, :, rows(c, k, by)]
            pltpu.make_async_copy(whole, whole, gr.at[k - 1, c, i]).wait()
            part = C.at[c, i, rows(c, k, by)]
            more.append(send(part, part, gs.at[k - 1, c, 2 + i], gr.at[k - 1, c, 2 + i], neighbour(me, p, dims[c][k], to)))
        return copies, more

    def gathered(k, c, copies, more):
        for i in range(2):
            part = C.at[c, i, rows(c, k, 2)]
            pltpu.make_async_copy(part, part, gr.at[k - 1, c, 2 + i]).wait()
        for copy in copies + more:
            copy.wait_send()

    copies = square(0)
    own = [spread(2, c) for c in range(3)]
    squared(0, copies)
    copies = square(1)
    more = [relay(2, c, own[c]) for c in range(3)]
    squared(1, copies)
    copies = square(2)
    for c in range(3):
        gathered(2, c, *more[c])
    own = [spread(1, c) for c in range(3)]
    squared(2, copies)
    copies = square(3)
    more = [relay(1, c, own[c]) for c in range(3)]
    squared(3, copies)
    factor[...] = jnp.full(factor.shape, jnp.minimum(1.0, 0.5 * lax.rsqrt(jnp.sum(sq[...], keepdims=True) / COUNT + 1e-30)), F32)
    stores = []
    for c in range(3):
        gathered(1, c, *more[c])
        stores.append(pltpu.make_async_copy(C.at[c], outs[c], osem.at[c]))
        stores[-1].start()
    for copy in list(swaps.values()) + sends:
        copy.wait_send()
    for store in stores:
        store.wait()


def reduce_all(g):
    dma, vmem = pltpu.SemaphoreType.DMA, pltpu.VMEM
    hbm = pl.BlockSpec(memory_space=pl.ANY)
    return pl.pallas_call(
        reduce_kernel,
        out_shape=[jax.ShapeDtypeStruct((2, 512, 512), BF16)] * 3 + [jax.ShapeDtypeStruct((8, 128), F32)],
        in_specs=[hbm] * 6,
        out_specs=[hbm] * 3 + [pl.BlockSpec(memory_space=pltpu.VMEM)],
        scratch_shapes=[
            vmem((3, 2, HALF, 512), BF16),
            vmem((3, 2, HALF, 512), BF16),
            vmem((3, 6, 2, 256, 512), BF16),
            vmem((3, 6, 2, 64, 512), BF16),
            vmem((3, 6, 2, 16, 512), BF16),
            vmem((3, 2, 512, 512), F32),
            vmem((3, 2, 128, 512), F32),
            vmem((3, 2, 512, 512), BF16),
            vmem((4, 4, 8, 128), F32),
            vmem((8, 128), F32),
            dma((3, 2)),
            dma((3, 4, 2)), dma((3, 4, 2)),
            dma((3, 3, 6)), dma((3, 3, 6)),
            dma((2, 3, 4)), dma((2, 3, 4)),
            dma((4, 3)), dma((4, 3)),
            dma((3,)),
        ],
        compiler_params=pltpu.CompilerParams(collective_id=1, has_side_effects=True, vmem_limit_bytes=60 * 2**20),
        name="reduce_all",
    )(*g)


def adamw_kernel(n_g, first, start, meta, f, *refs):
    unit = pl.program_id(0)
    ins, refs = refs[:9], refs[9:]
    g, refs = refs[: 3 * n_g], refs[3 * n_g :]
    outs = refs if first else refs[9:]
    outs[9][...] = jnp.zeros_like(outs[9])
    factor = f[0, 0]

    def update(c, gref):
        w, m, v = ins[c], ins[3 + c], ins[6 + c]
        ow, om, ov = outs[c], outs[3 + c], outs[6 + c]
        for half in range(2):
            def body(i, carry):
                if c < 2:
                    at = (0, pl.ds(half * 32, 32), pl.ds(pl.multiple_of(i * 512, 512), 512))
                else:
                    at = (0, pl.ds(pl.multiple_of(half * 256 + i * 32, 32), 32), slice(None))
                wide = gref[0, half * 8 + i].astype(F32) * factor
                nm = 0.9 * m[at] + 0.1 * wide
                nv = 0.95 * v[at] + 0.05 * wide * wide
                old = w[at].astype(F32)
                om[at] = nm
                ov[at] = nv
                ow[at] = (old - 0.02 * (nm * lax.rsqrt(nv + 1e-8) + 0.1 * old)).astype(BF16)
                return carry

            lax.fori_loop(0, 8, body, 0, unroll=2)

    for k in range(n_g):
        @pl.when(unit == k)
        def _():
            for c in range(3):
                update(c, g[3 * k + c])


def adamw_part(meta, start, units, f, state, so_far):
    n_g = len(units)

    def rows(c):
        return lambda u, meta: (meta[start + u, 3], meta[start + u, c], 0)

    wide, tall = (1, 64, 4096), (1, 512, 512)
    state_specs = [pl.BlockSpec(tall if c == 2 else wide, rows(c)) for _ in range(3) for c in range(3)]
    grads, grad_specs = [], []
    for arrays, index in units:
        for c in range(3):
            grads.append(arrays[c].reshape(arrays[c].shape[0], 16, 32, 512))
            grad_specs.append(pl.BlockSpec((1, 16, 32, 512), lambda u, meta, index=index: (index, 0, 0, 0)))
    before = [] if so_far is None else list(so_far)
    shapes = [jax.ShapeDtypeStruct(a.shape, a.dtype) for a in state] + [jax.ShapeDtypeStruct((8, 128), F32)]
    elements = n_g * 3 * 262144
    return pl.pallas_call(
        functools.partial(adamw_kernel, n_g, so_far is None, start),
        out_shape=shapes,
        grid_spec=pltpu.PrefetchScalarGridSpec(
            num_scalar_prefetch=1,
            grid=(n_g,),
            in_specs=[pl.BlockSpec((8, 128), lambda u, meta: (0, 0), memory_space=pltpu.SMEM)] + state_specs + grad_specs + [pl.BlockSpec(memory_space=pl.ANY)] * len(before),
            out_specs=state_specs + [pl.BlockSpec((8, 128), lambda u, meta: (0, 0))],
        ),
        input_output_aliases={2 + 9 + 3 * n_g + i: i for i in range(len(before))},
        compiler_params=pltpu.CompilerParams(dimension_semantics=("arbitrary",), vmem_limit_bytes=62 * 2**20),
        cost_estimate=pl.CostEstimate(flops=elements * 400, bytes_accessed=elements * 22, transcendentals=elements),
        name="adamw",
    )(meta, f, *state, *grads, *before)


def ring(d, by):
    return [(i, i + ((i // STRIDE[d] % 4 + by) % 4 - i // STRIDE[d] % 4) * STRIDE[d]) for i in range(128)]


PARTNER = [(i, i ^ 1) for i in range(128)]


def finish(g, weights, m, v):
    c0, c1, c2, f = reduce_all([g[c][l] for c in range(3) for l in range(2)])
    own = (c0, c1, c2)

    def swap(arrays):
        return [lax.ppermute(a, "dp", PARTNER) for a in arrays]

    after = [lax.ppermute(own[c], "dp", ring(c, 3)) for c in range(3)]
    ahead = [lax.ppermute(own[c], "dp", ring(c, 1)) for c in range(3)]
    own_x = swap(own)

    me, core, p = place()
    order = [(0, 0), (0, 1), (1, 0), (3, 0), (1, 1), (3, 1), (2, 0), (2, 1)]
    flip = jnp.array([other for _, other in order], jnp.int32)
    by = jnp.array([by for by, _ in order], jnp.int32)
    first = (core ^ flip) * 4
    meta = jnp.stack([first + lax.rem(p[c] + by, 4) for c in range(3)], -1)
    meta = jnp.concatenate([jnp.repeat(meta, 2, 0), jnp.array([[l] for _ in order for l in range(2)], jnp.int32)], -1)

    def both(*sets):
        return [(arrays, l) for arrays in sets for l in range(2)]

    def held(arrays, token):
        return [lax.optimization_barrier((a, token))[0] for a in arrays]

    state = [*weights, *m, *v]
    *so_far, token = adamw_part(meta, 0, both(own), f, state, None)
    *so_far, token = adamw_part(meta, 2, both(own_x), f, state, so_far)
    after_held, ahead_held = held(after, token), held(ahead, token)
    far = [lax.ppermute(after_held[c], "dp", ring(c, 3)) for c in range(3)]
    after_x, ahead_x = swap(after_held), swap(ahead_held)
    *so_far, token = adamw_part(meta, 4, both(after, ahead), f, state, so_far)
    far_x = swap(held(far, token))
    *so_far, token = adamw_part(meta, 8, both(after_x, ahead_x, far), f, state, so_far)
    *so_far, token = adamw_part(meta, 14, both(far_x), f, state, so_far)
    return tuple(so_far)


def solution(mesh):
    def step(x, dy, *arrays):
        weights, m, v = (arrays[i : i + 3] for i in (0, 3, 6))
        return finish(terms(x[0], dy[0], *weights), weights, m, v)

    return jax.shard_map(
        step,
        mesh=mesh,
        in_specs=(P(("rep", "dp"), None, None),) * 2 + (P(None, None, None),) * 9,
        out_specs=(P("rep", None, None),) * 9,
        check_vma=False,
    )
```

```python
import functools

import jax
import jax.numpy as jnp
from jax import lax
from jax.experimental import pallas as pl
from jax.experimental.pallas import tpu as pltpu
from jax.sharding import PartitionSpec as P

COUNT = 2 * 3 * 512 * 4096
F32, BF16 = jnp.float32, jnp.bfloat16
STRIDE = (32, 8, 2)


ROWS, TILE, CHUNK, PIECE = 1024, 512, 512, 32


def dot(a, b, dims=((1,), (0,))):
    return lax.dot_general(a, b, (dims, ((), ())), preferred_element_type=F32)


def norm_into(h_ref, a, scale=None):
    for r in range(0, ROWS, 128):
        wide = h_ref[r : r + 128, :].astype(F32)
        by = lax.rsqrt(jnp.mean(wide * wide, -1, keepdims=True) + 1e-6)
        a[r : r + 128, :] = (wide * by).astype(BF16)
        if scale is not None:
            scale[r : r + 128, :] = jnp.broadcast_to(by, (128, 128))


def flip_into(a, t):
    for r in range(0, ROWS, 256):
        t[:, r : r + 256] = a[r : r + 256, :].T


def weave(pieces, dots):
    n = max(len(pieces), len(dots))
    for i in range(n):
        for steps in (pieces, dots):
            for step in steps[i * len(steps) // n : (i + 1) * len(steps) // n]:
                step()


def forward_kernel(x, wg, wu, wd, gate, up, h1, a, s, acc):
    j = pl.program_id(0)

    @pl.when(j == 0)
    def _():
        norm_into(x, a)
        acc[...] = jnp.zeros_like(acc)

    def product(i):
        g = gate[i : i + PIECE, :]
        s[i : i + PIECE, :] = (g * jax.nn.sigmoid(g) * up[i : i + PIECE, :]).astype(BF16)

    def down(r, n):
        acc[r : r + CHUNK, n : n + 256] += dot(s[r : r + CHUNK, :], wd[0, :, n : n + 256])

    def start(r, w, out, n):
        out[r : r + CHUNK, n : n + 256] = dot(a[r : r + CHUNK, :], w[0, :, n : n + 256])

    for r in range(0, ROWS + 2 * CHUNK, CHUNK):
        pieces, dots = [], []
        if CHUNK <= r <= ROWS:
            pieces = [functools.partial(product, i) for i in range(r - CHUNK, r, PIECE)]
        if r < ROWS:
            dots += [functools.partial(start, r, w, out, n) for n in (0, 256) for w, out in ((wg, gate), (wu, up))]
        if r >= 2 * CHUNK:
            dots += [functools.partial(down, r - 2 * CHUNK, n) for n in (0, 256)]
        weave(pieces, dots)

    @pl.when(j == pl.num_programs(0) - 1)
    def _():
        for r in range(0, ROWS, 128):
            h1[r : r + 128, :] = x[r : r + 128, :] + acc[r : r + 128, :].astype(BF16)


def gated(g, u, d):
    sig = jax.nn.sigmoid(g)
    silu = g * sig
    d = d.astype(BF16).astype(F32)
    du = d * silu
    ds = d * u
    return (silu * u).astype(BF16), (ds * sig + ds * g * (sig * (1.0 - sig))).astype(BF16), du.astype(BF16)


def backward(tokens, gradients, at, yt, s, dg, du, fg, fu, fd, gate, up, ds, og, ou, od):
    def product(i):
        k = slice(i, i + PIECE)
        s[k, :], dg[k, :], du[k, :] = gated(gate[k, :], up[k, :], ds[k, :])

    def term(r, left, right, out, n):
        here = dot(left[:, r : r + CHUNK], right[r : r + CHUNK, n : n + 256])
        out[:, n : n + 256] = here if r == 0 else out[:, n : n + 256] + here

    for r in range(0, ROWS + 2 * CHUNK, CHUNK):
        pieces, dots = [], []
        if CHUNK <= r <= ROWS:
            pieces = [functools.partial(product, i) for i in range(r - CHUNK, r, PIECE)]
        if r >= 2 * CHUNK:
            q = r - 2 * CHUNK
            dots += gradients(q) + [functools.partial(term, q, left, right, out, n) for left, right, out in ((at, dg, fg), (at, du, fu), (yt, s, fd)) for n in (0, 256)]
        if r < ROWS:
            dots += tokens(r)
        weave(pieces, dots)
    og[:, 0] = fg[...].astype(BF16).reshape(16, 32, TILE)
    ou[:, 0] = fu[...].astype(BF16).reshape(16, 32, TILE)
    od[...] = fd[...].astype(BF16).T


def last_kernel(h1, dy, wg, wu, wd, og, ou, od, dh, a, at, yt, s, dg, du, fg, fu, fd, gate, up, ds, accg, accu, scale):
    j = pl.program_id(0)

    @pl.when(j == 0)
    def _():
        norm_into(h1, a, scale)
        flip_into(a, at)
        flip_into(dy, yt)
        accg[...] = jnp.zeros_like(accg)
        accu[...] = jnp.zeros_like(accu)

    def start(r, left, w, out, n):
        rows = slice(r, r + CHUNK)
        if out is ds:
            out[rows, n : n + 256] = dot(left[rows, :], w[0, n : n + 256, :], ((1,), (1,)))
        else:
            out[rows, n : n + 256] = dot(left[rows, :], w[0, :, n : n + 256])

    def add(r, left, w, out, n):
        rows = slice(r, r + CHUNK)
        out[rows, n : n + 256] += dot(left[rows, :], w[0, n : n + 256, :], ((1,), (1,)))

    backward(
        lambda r: [functools.partial(start, r, *which, n) for which in ((a, wg, gate), (a, wu, up), (dy, wd, ds)) for n in (0, 256)],
        lambda r: [functools.partial(add, r, *which, n) for which in ((dg, wg, accg), (du, wu, accu)) for n in (0, 256)],
        at, yt, s, dg, du, fg, fu, fd, gate, up, ds, og, ou, od,
    )

    @pl.when(j == pl.num_programs(0) - 1)
    def _():
        for r in range(0, ROWS, 64):
            k = slice(r, r + 64)
            by_a = (accg[k, :].astype(BF16) + accu[k, :].astype(BF16)).astype(F32)
            wide = h1[k, :].astype(F32)
            by = scale[k, :1]
            by_scale = jnp.sum(by_a * wide, -1, keepdims=True)
            by_wide = by_a * by + wide * (by_scale * (by * by * by) * (-1.0 / 512))
            dh[k, :] = dy[k, :] + by_wide.astype(BF16)


def weight_gradients(at, yt, s, dg, du, og, ou, od):
    for half in range(2):
        rows = slice(half * 256, half * 256 + 256)
        og[half * 8 : half * 8 + 8, 0] = dot(at[rows, :], dg[...]).astype(BF16).reshape(8, 32, TILE)
        ou[half * 8 : half * 8 + 8, 0] = dot(at[rows, :], du[...]).astype(BF16).reshape(8, 32, TILE)
        od[:, rows] = dot(yt[rows, :], s[...]).astype(BF16).T


def first_kernel(x, dy, wd, gate, up, og, ou, od, a, at, yt, s, dg, du, ds):
    j = pl.program_id(0)

    @pl.when(j == 0)
    def _():
        norm_into(x, a)
        flip_into(a, at)
        flip_into(dy, yt)

    for r in range(0, ROWS, CHUNK):
        rows = pl.ds(r, CHUNK)
        ds[rows, :] = dot(dy[rows, :], wd[0], ((1,), (1,)))
        for i in range(r, r + CHUNK, PIECE):
            k = slice(i, i + PIECE)
            s[k, :], dg[k, :], du[k, :] = gated(gate[k, :], up[k, :], ds[k, :])
    weight_gradients(at, yt, s, dg, du, og, ou, od)


def terms(x, dy, w_gate, w_up, w_down):
    vmem = pltpu.VMEM
    steps = 4096 // TILE
    full = pl.BlockSpec((ROWS, 512), lambda j: (0, 0))
    tile = pl.BlockSpec((ROWS, TILE), lambda j: (0, j))
    shape = jax.ShapeDtypeStruct
    states, wide = shape((ROWS, 512), BF16), shape((ROWS, 4096), F32)

    def weight(l):
        return [pl.BlockSpec((1, 512, TILE), lambda j: (l, 0, j))] * 2 + [pl.BlockSpec((1, TILE, 512), lambda j: (l, j, 0))]

    grads = [shape((16, 8, 32, TILE), BF16)] * 2 + [shape((4096, 512), BF16)]
    grad_specs = [pl.BlockSpec((16, 1, 32, TILE), lambda j: (0, j, 0, 0))] * 2 + [pl.BlockSpec((TILE, 512), lambda j: (j, 0))]
    b, t, f = vmem((ROWS, 512), BF16), vmem((512, ROWS), BF16), vmem((ROWS, 512), F32)
    o = vmem((512, TILE), F32)

    def call(kernel, dots, name, out_shape, in_specs, out_specs, scratch, *args):
        return pl.pallas_call(
            kernel, out_shape=out_shape, grid=(steps,), in_specs=in_specs, out_specs=out_specs, scratch_shapes=scratch, name=name,
            compiler_params=pltpu.CompilerParams(dimension_semantics=("arbitrary",), vmem_limit_bytes=60 * 2**20),
            cost_estimate=pl.CostEstimate(flops=dots * 2 * 1024 * 512 * 4096, bytes_accessed=30 * 2**20, transcendentals=2**22),
        )(*args)

    gate, up, h1 = call(forward_kernel, 3, "forward", [wide, wide, states], [full] + weight(0), [tile, tile, full], [b, b, f], x, w_gate, w_up, w_down)
    g1 = call(last_kernel, 8, "last", grads + [states], [full, full] + weight(1), grad_specs + [full],
              [b, t, t, b, b, b, o, o, o, f, f, f, f, f, vmem((ROWS, 128), F32)], h1, dy, w_gate, w_up, w_down)
    *g1, dh = g1
    g0 = call(first_kernel, 4, "first", grads, [full, full, weight(0)[2], tile, tile], grad_specs, [b, t, t, b, b, b, f], x, dh, w_down, gate, up)
    return [[g[c].reshape(4096, 512) for g in (g0, g1)] for c in range(3)]


def place():
    me = lax.axis_index("dp")
    return me, lax.rem(me, 2), [lax.rem(lax.div(me, s), 4) for s in STRIDE]


def neighbour(me, p, d, by):
    return me + (lax.rem(p[d] + by, 4) - p[d]) * STRIDE[d]


HALF, SIZES = 2048, (512, 128, 32)


def reduce_kernel(g00, g01, g10, g11, g20, g21, c0, c1, c2, factor, H, R0, R1, R2, R3, F1, F2, C, N, sq,
                  lsem, ds, dr, ps, pr, gs, gr, ns, nr, osem):
    g, outs = ((g00, g01), (g10, g11), (g20, g21)), (c0, c1, c2)
    me, core, p = place()
    partner = me + 1 - 2 * core
    dims = [(c, (c + 1) % 3, (c + 2) % 3) for c in range(3)]

    def send(src, dst, s, r, to):
        copy = pltpu.make_async_remote_copy(src_ref=src, dst_ref=dst, send_sem=s, recv_sem=r, device_id={"dp": to}, device_id_type=pl.DeviceIdType.MESH)
        copy.start()
        return copy

    barrier = pltpu.get_barrier_semaphore()
    others = [partner] + [neighbour(me, p, d, by) for d in range(3) for by in (1, 2, 3)]
    for other in others:
        pl.semaphore_signal(barrier, inc=1, device_id={"dp": other}, device_id_type=pl.DeviceIdType.MESH)

    loads = [pltpu.make_async_copy(g[c][l].at[pl.ds(pl.multiple_of(core * HALF, HALF), HALF)], H.at[c, l], lsem.at[c, l]) for c in range(3) for l in range(2)]
    for l in (1, 0):
        for c in range(3):
            loads[2 * c + l].start()
    pl.semaphore_wait(barrier, len(others))

    swaps = {}
    for l in (1, 0):
        for by in (2, 3, 1, 0):
            for c in range(3):
                at = pl.multiple_of(lax.rem(p[c] + by, 4) * 512, 512)
                swaps[c, by, l] = send(g[c][l].at[pl.ds(pl.multiple_of((1 - core) * HALF, HALF) + at, 512)], R0.at[c, l, pl.ds(at, 512)], ds.at[c, by, l], dr.at[c, by, l], partner)

    sends = []
    received = (R1, R2, R3)

    def term(k, c, l, at, row, step):
        rows = pl.ds(pl.multiple_of(at + row, 16), step)
        if k == 0:
            return H[c, l, rows].astype(F32) + R0[c, l, rows].astype(F32)
        return (F1, F2)[k - 1][c, l, rows]

    def make(k, c, l, at, slots, keep):
        half = SIZES[k] // 2
        step = min(half, 32)

        def body(i, carry):
            row = pl.multiple_of(i * step, 16)
            total = term(k, c, l, at, row, step)
            for slot in slots:
                total += received[k][c, slot, l, pl.ds(row, step)].astype(F32)
            keep(row, step, total)
            return carry

        lax.fori_loop(0, half // step, body, 0)

    def leave(k, c, l, by, side, slots, to, slot):
        half = SIZES[k] // 2
        at = pl.multiple_of(lax.rem(p[dims[c][k]] + by, 4) * SIZES[k] + side * half, 16)
        base = pl.multiple_of(sum((p[dims[c][i]] * SIZES[i] for i in range(k)), at), 16)

        def keep(row, step, total):
            H[c, l, pl.ds(pl.multiple_of(base + row, 16), step)] = total.astype(BF16)

        make(k, c, l, at, slots, keep)
        sends.append(send(H.at[c, l, pl.ds(base, half)], received[k].at[c, slot, l], ps.at[k, c, slot, l], pr.at[k, c, slot, l], neighbour(me, p, dims[c][k], to)))

    def arrived(k, c, l, slot):
        here = received[k].at[c, slot, l]
        pltpu.make_async_copy(here, here, pr.at[k, c, slot, l]).wait()

    def far(k, l):
        for c in range(3):
            if k == 0:
                loads[2 * c + l].wait()
                swaps[c, 2, l].wait_recv()
            leave(k, c, l, 2, 0, (), 3, 0)
            leave(k, c, l, 2, 1, (), 1, 3)

    def near(k, l):
        for c in range(3):
            if k == 0:
                swaps[c, 3, l].wait_recv(), swaps[c, 1, l].wait_recv()
            leave(k, c, l, 3, 1, (), 3, 1)
            leave(k, c, l, 1, 0, (), 1, 4)

    def onward(k, l):
        for c in range(3):
            arrived(k, c, l, 0)
            leave(k, c, l, 3, 0, (0,), 3, 2)
            arrived(k, c, l, 3)
            leave(k, c, l, 1, 1, (3,), 1, 5)

    def mine(k, l):
        half = SIZES[k] // 2
        for c in range(3):
            if k == 0:
                swaps[c, 0, l].wait_recv()
            for slot in (1, 4, 2, 5):
                arrived(k, c, l, slot)
            for side, slots in ((0, (2, 4)), (1, (1, 5))):
                at = pl.multiple_of(p[dims[c][k]] * SIZES[k] + side * half, 16)

                def keep(row, step, total):
                    if k < 2:
                        (F1, F2)[k][c, l, pl.ds(pl.multiple_of(side * half + row, 16), step)] = total
                    else:
                        rounded = total.astype(BF16)
                        C[c, l, pl.ds(pl.multiple_of(p[dims[c][1]] * 128 + p[dims[c][2]] * 32 + side * half, 16), step)] = rounded
                        wide = rounded.astype(F32)
                        wide = wide * wide
                        sq[...] += sum(wide[8 * a : 8 * a + 8, 128 * b : 128 * b + 128] for a in range(step // 8) for b in range(4))

                make(k, c, l, at, slots, keep)

    def square(n):
        to = [partner] if n == 0 else [neighbour(me, p, n - 1, by) for by in (1, 2, 3)]
        own = core if n == 0 else p[n - 1]
        N[n, own] = sq[...]
        return [send(sq, N.at[n, own], ns.at[n, i], nr.at[n, i], dev) for i, dev in enumerate(to)]

    def squared(n, copies):
        for copy in copies:
            copy.wait()
        sq[...] = N[n, 0] + N[n, 1] if n == 0 else (N[n, 0] + N[n, 1]) + (N[n, 2] + N[n, 3])

    def rows(c, k, by, side=None):
        at = lax.rem(p[dims[c][k]] + by, 4) * SIZES[k] + (p[dims[c][1]] * 128 if k == 2 else 0)
        if side is None:
            return pl.ds(pl.multiple_of(at, 32), SIZES[k])
        return pl.ds(pl.multiple_of(at + side * (SIZES[k] // 2), 16), SIZES[k] // 2)

    def spread(k, l):
        for c in range(3):
            own = C.at[c, l, rows(c, k, 0)]
            for i, to in ((0, 3), (1, 1)):
                sends.append(send(own, own, gs.at[k - 1, c, i, l], gr.at[k - 1, c, i, l], neighbour(me, p, dims[c][k], to)))

    def relay(k, l):
        for c in range(3):
            for i, by, to in ((0, 1, 3), (1, 3, 1)):
                whole = C.at[c, l, rows(c, k, by)]
                pltpu.make_async_copy(whole, whole, gr.at[k - 1, c, i, l]).wait()
                part = C.at[c, l, rows(c, k, by, i)]
                sends.append(send(part, part, gs.at[k - 1, c, 2 + i, l], gr.at[k - 1, c, 2 + i, l], neighbour(me, p, dims[c][k], to)))

    def gathered(k, l):
        for c in range(3):
            for i in range(2):
                part = C.at[c, l, rows(c, k, 2, i)]
                pltpu.make_async_copy(part, part, gr.at[k - 1, c, 2 + i, l]).wait()

    stores = []

    def store(l):
        for c in range(3):
            stores.append(pltpu.make_async_copy(C.at[c, l], outs[c].at[l], osem.at[c, l]))
            stores[-1].start()

    sq[...] = jnp.zeros_like(sq)
    far(0, 1), near(0, 1), onward(0, 1)
    far(0, 0), near(0, 0)
    mine(0, 1), far(1, 1), near(1, 1)
    onward(0, 0)
    onward(1, 1)
    mine(1, 1), far(2, 1), near(2, 1)
    mine(0, 0), far(1, 0), near(1, 0)
    onward(2, 1)
    onward(1, 0)
    mine(2, 1), spread(2, 1)
    mine(1, 0), far(2, 0), near(2, 0)
    relay(2, 1)
    onward(2, 0)
    gathered(2, 1), spread(1, 1)
    mine(2, 0)
    copies = square(0)
    spread(2, 0)
    squared(0, copies)
    copies = square(1)
    relay(2, 0)
    relay(1, 1)
    squared(1, copies)
    copies = square(2)
    gathered(2, 0), spread(1, 0)
    squared(2, copies)
    copies = square(3)
    gathered(1, 1), store(1)
    relay(1, 0)
    squared(3, copies)
    factor[...] = jnp.full(factor.shape, jnp.minimum(1.0, 0.5 * lax.rsqrt(jnp.sum(sq[...], keepdims=True) / COUNT + 1e-30)), F32)
    gathered(1, 0), store(0)
    for copy in list(swaps.values()) + sends:
        copy.wait_send()
    for copy in stores:
        copy.wait()


def reduce_all(g):
    dma, vmem = pltpu.SemaphoreType.DMA, pltpu.VMEM
    hbm = pl.BlockSpec(memory_space=pl.ANY)
    return pl.pallas_call(
        reduce_kernel,
        out_shape=[jax.ShapeDtypeStruct((2, 512, 512), BF16)] * 3 + [jax.ShapeDtypeStruct((8, 128), F32)],
        in_specs=[hbm] * 6,
        out_specs=[hbm] * 3 + [pl.BlockSpec(memory_space=pltpu.VMEM)],
        scratch_shapes=[
            vmem((3, 2, HALF, 512), BF16),
            vmem((3, 2, HALF, 512), BF16),
            vmem((3, 6, 2, 256, 512), BF16),
            vmem((3, 6, 2, 64, 512), BF16),
            vmem((3, 6, 2, 16, 512), BF16),
            vmem((3, 2, 512, 512), F32),
            vmem((3, 2, 128, 512), F32),
            vmem((3, 2, 512, 512), BF16),
            vmem((4, 4, 8, 128), F32),
            vmem((8, 128), F32),
            dma((3, 2)),
            dma((3, 4, 2)), dma((3, 4, 2)),
            dma((3, 3, 6, 2)), dma((3, 3, 6, 2)),
            dma((2, 3, 4, 2)), dma((2, 3, 4, 2)),
            dma((4, 3)), dma((4, 3)),
            dma((3, 2)),
        ],
        compiler_params=pltpu.CompilerParams(collective_id=1, has_side_effects=True, vmem_limit_bytes=60 * 2**20),
        name="reduce_all",
    )(*g)


def adamw_kernel(n_g, first, start, meta, f, *refs):
    unit = pl.program_id(0)
    ins, refs = refs[:9], refs[9:]
    g, refs = refs[: 3 * n_g], refs[3 * n_g :]
    outs = refs if first else refs[9:]
    outs[9][...] = jnp.zeros_like(outs[9])
    factor = f[0, 0]

    def update(c, gref):
        w, m, v = ins[c], ins[3 + c], ins[6 + c]
        ow, om, ov = outs[c], outs[3 + c], outs[6 + c]
        for half in range(2):
            def body(i, carry):
                if c < 2:
                    at = (0, pl.ds(half * 32, 32), pl.ds(pl.multiple_of(i * 512, 512), 512))
                else:
                    at = (0, pl.ds(pl.multiple_of(half * 256 + i * 32, 32), 32), slice(None))
                wide = gref[0, half * 8 + i].astype(F32) * factor
                nm = 0.9 * m[at] + 0.1 * wide
                nv = 0.95 * v[at] + 0.05 * wide * wide
                old = w[at].astype(F32)
                om[at] = nm
                ov[at] = nv
                ow[at] = (old - 0.02 * (nm * lax.rsqrt(nv + 1e-8) + 0.1 * old)).astype(BF16)
                return carry

            lax.fori_loop(0, 8, body, 0, unroll=2)

    for k in range(n_g):
        @pl.when(unit == k)
        def _():
            for c in range(3):
                update(c, g[3 * k + c])


def adamw_part(meta, start, units, f, state, so_far):
    n_g = len(units)

    def rows(c):
        return lambda u, meta: (meta[start + u, 3], meta[start + u, c], 0)

    wide, tall = (1, 64, 4096), (1, 512, 512)
    state_specs = [pl.BlockSpec(tall if c == 2 else wide, rows(c)) for _ in range(3) for c in range(3)]
    grads, grad_specs = [], []
    for arrays, index in units:
        for c in range(3):
            grads.append(arrays[c].reshape(arrays[c].shape[0], 16, 32, 512))
            grad_specs.append(pl.BlockSpec((1, 16, 32, 512), lambda u, meta, index=index: (index, 0, 0, 0)))
    before = [] if so_far is None else list(so_far)
    shapes = [jax.ShapeDtypeStruct(a.shape, a.dtype) for a in state] + [jax.ShapeDtypeStruct((8, 128), F32)]
    elements = n_g * 3 * 262144
    return pl.pallas_call(
        functools.partial(adamw_kernel, n_g, so_far is None, start),
        out_shape=shapes,
        grid_spec=pltpu.PrefetchScalarGridSpec(
            num_scalar_prefetch=1,
            grid=(n_g,),
            in_specs=[pl.BlockSpec((8, 128), lambda u, meta: (0, 0), memory_space=pltpu.SMEM)] + state_specs + grad_specs + [pl.BlockSpec(memory_space=pl.ANY)] * len(before),
            out_specs=state_specs + [pl.BlockSpec((8, 128), lambda u, meta: (0, 0))],
        ),
        input_output_aliases={2 + 9 + 3 * n_g + i: i for i in range(len(before))},
        compiler_params=pltpu.CompilerParams(dimension_semantics=("arbitrary",), vmem_limit_bytes=62 * 2**20),
        cost_estimate=pl.CostEstimate(flops=elements * 400, bytes_accessed=elements * 22, transcendentals=elements),
        name="adamw",
    )(meta, f, *state, *grads, *before)


def ring(d, by):
    return [(i, i + ((i // STRIDE[d] % 4 + by) % 4 - i // STRIDE[d] % 4) * STRIDE[d]) for i in range(128)]


PARTNER = [(i, i ^ 1) for i in range(128)]


def finish(g, weights, m, v):
    c0, c1, c2, f = reduce_all([g[c][l] for c in range(3) for l in range(2)])
    own = (c0, c1, c2)

    def swap(arrays):
        return [lax.ppermute(a, "dp", PARTNER) for a in arrays]

    after = [lax.ppermute(own[c], "dp", ring(c, 3)) for c in range(3)]
    ahead = [lax.ppermute(own[c], "dp", ring(c, 1)) for c in range(3)]
    own_x = swap(own)

    me, core, p = place()
    order = [(0, 0), (0, 1), (1, 0), (3, 0), (1, 1), (3, 1), (2, 0), (2, 1)]
    flip = jnp.array([other for _, other in order], jnp.int32)
    by = jnp.array([by for by, _ in order], jnp.int32)
    first = (core ^ flip) * 4
    meta = jnp.stack([first + lax.rem(p[c] + by, 4) for c in range(3)], -1)
    meta = jnp.concatenate([jnp.repeat(meta, 2, 0), jnp.array([[l] for _ in order for l in range(2)], jnp.int32)], -1)

    def both(*sets):
        return [(arrays, l) for arrays in sets for l in range(2)]

    def held(arrays, token):
        return [lax.optimization_barrier((a, token))[0] for a in arrays]

    state = [*weights, *m, *v]
    *so_far, token = adamw_part(meta, 0, both(own), f, state, None)
    *so_far, token = adamw_part(meta, 2, both(own_x), f, state, so_far)
    after_held, ahead_held = held(after, token), held(ahead, token)
    far = [lax.ppermute(after_held[c], "dp", ring(c, 3)) for c in range(3)]
    after_x, ahead_x = swap(after_held), swap(ahead_held)
    *so_far, token = adamw_part(meta, 4, both(after, ahead), f, state, so_far)
    far_x = swap(held(far, token))
    *so_far, token = adamw_part(meta, 8, both(after_x, ahead_x, far), f, state, so_far)
    *so_far, token = adamw_part(meta, 14, both(far_x), f, state, so_far)
    return tuple(so_far)


def solution(mesh):
    def step(x, dy, *arrays):
        weights, m, v = (arrays[i : i + 3] for i in (0, 3, 6))
        return finish(terms(x[0], dy[0], *weights), weights, m, v)

    return jax.shard_map(
        step,
        mesh=mesh,
        in_specs=(P(("rep", "dp"), None, None),) * 2 + (P(None, None, None),) * 9,
        out_specs=(P("rep", None, None),) * 9,
        check_vma=False,
    )
```

```python
import functools

import jax
import jax.numpy as jnp
from jax import lax
from jax.experimental import pallas as pl
from jax.experimental.pallas import tpu as pltpu
from jax.sharding import PartitionSpec as P

COUNT = 2 * 3 * 512 * 4096
F32, BF16 = jnp.float32, jnp.bfloat16
STRIDE = (32, 8, 2)


ROWS, TILE, CHUNK, PIECE = 1024, 512, 512, 32


def dot(a, b, dims=((1,), (0,))):
    return lax.dot_general(a, b, (dims, ((), ())), preferred_element_type=F32)


def norm_into(h_ref, a, scale=None):
    for r in range(0, ROWS, 128):
        wide = h_ref[r : r + 128, :].astype(F32)
        by = lax.rsqrt(jnp.mean(wide * wide, -1, keepdims=True) + 1e-6)
        a[r : r + 128, :] = (wide * by).astype(BF16)
        if scale is not None:
            scale[r : r + 128, :] = jnp.broadcast_to(by, (128, 128))


def flip_into(a, t):
    for r in range(0, ROWS, 256):
        t[:, r : r + 256] = a[r : r + 256, :].T


def weave(pieces, dots):
    n = max(len(pieces), len(dots))
    for i in range(n):
        for steps in (pieces, dots):
            for step in steps[i * len(steps) // n : (i + 1) * len(steps) // n]:
                step()


def forward_kernel(x, wg, wu, wd, gate, up, h1, a, s, acc):
    j = pl.program_id(0)

    @pl.when(j == 0)
    def _():
        norm_into(x, a)
        acc[...] = jnp.zeros_like(acc)

    def product(i):
        g = gate[i : i + PIECE, :]
        s[i : i + PIECE, :] = (g * jax.nn.sigmoid(g) * up[i : i + PIECE, :]).astype(BF16)

    def down(r, n):
        acc[r : r + CHUNK, n : n + 256] += dot(s[r : r + CHUNK, :], wd[0, :, n : n + 256])

    def start(r, w, out, n):
        out[r : r + CHUNK, n : n + 256] = dot(a[r : r + CHUNK, :], w[0, :, n : n + 256])

    for r in range(0, ROWS + 2 * CHUNK, CHUNK):
        pieces, dots = [], []
        if CHUNK <= r <= ROWS:
            pieces = [functools.partial(product, i) for i in range(r - CHUNK, r, PIECE)]
        if r < ROWS:
            dots += [functools.partial(start, r, w, out, n) for n in (0, 256) for w, out in ((wg, gate), (wu, up))]
        if r >= 2 * CHUNK:
            dots += [functools.partial(down, r - 2 * CHUNK, n) for n in (0, 256)]
        weave(pieces, dots)

    @pl.when(j == pl.num_programs(0) - 1)
    def _():
        for r in range(0, ROWS, 128):
            h1[r : r + 128, :] = x[r : r + 128, :] + acc[r : r + 128, :].astype(BF16)


def gated(g, u, d):
    sig = jax.nn.sigmoid(g)
    silu = g * sig
    d = d.astype(BF16).astype(F32)
    du = d * silu
    ds = d * u
    return (silu * u).astype(BF16), (ds * sig + ds * g * (sig * (1.0 - sig))).astype(BF16), du.astype(BF16)


def backward(tokens, gradients, at, yt, s, dg, du, fg, fu, fd, gate, up, ds, og, ou, od):
    def product(i):
        k = slice(i, i + PIECE)
        s[k, :], dg[k, :], du[k, :] = gated(gate[k, :], up[k, :], ds[k, :])

    def term(r, left, right, out, n):
        here = dot(left[:, r : r + CHUNK], right[r : r + CHUNK, n : n + 256])
        out[:, n : n + 256] = here if r == 0 else out[:, n : n + 256] + here

    for r in range(0, ROWS + 2 * CHUNK, CHUNK):
        pieces, dots = [], []
        if CHUNK <= r <= ROWS:
            pieces = [functools.partial(product, i) for i in range(r - CHUNK, r, PIECE)]
        if r >= 2 * CHUNK:
            q = r - 2 * CHUNK
            dots += gradients(q) + [functools.partial(term, q, left, right, out, n) for left, right, out in ((at, dg, fg), (at, du, fu), (yt, s, fd)) for n in (0, 256)]
        if r < ROWS:
            dots += tokens(r)
        weave(pieces, dots)
    og[:, 0] = fg[...].astype(BF16).reshape(16, 32, TILE)
    ou[:, 0] = fu[...].astype(BF16).reshape(16, 32, TILE)
    od[...] = fd[...].astype(BF16).T


def last_kernel(h1, dy, wg, wu, wd, og, ou, od, dh, a, at, yt, s, dg, du, fg, fu, fd, gate, up, ds, accg, accu, scale):
    j = pl.program_id(0)

    @pl.when(j == 0)
    def _():
        norm_into(h1, a, scale)
        flip_into(a, at)
        flip_into(dy, yt)
        accg[...] = jnp.zeros_like(accg)
        accu[...] = jnp.zeros_like(accu)

    def start(r, left, w, out, n):
        rows = slice(r, r + CHUNK)
        if out is ds:
            out[rows, n : n + 256] = dot(left[rows, :], w[0, n : n + 256, :], ((1,), (1,)))
        else:
            out[rows, n : n + 256] = dot(left[rows, :], w[0, :, n : n + 256])

    def add(r, left, w, out, n):
        rows = slice(r, r + CHUNK)
        out[rows, n : n + 256] += dot(left[rows, :], w[0, n : n + 256, :], ((1,), (1,)))

    backward(
        lambda r: [functools.partial(start, r, *which, n) for which in ((a, wg, gate), (a, wu, up), (dy, wd, ds)) for n in (0, 256)],
        lambda r: [functools.partial(add, r, *which, n) for which in ((dg, wg, accg), (du, wu, accu)) for n in (0, 256)],
        at, yt, s, dg, du, fg, fu, fd, gate, up, ds, og, ou, od,
    )

    @pl.when(j == pl.num_programs(0) - 1)
    def _():
        for r in range(0, ROWS, 64):
            k = slice(r, r + 64)
            by_a = (accg[k, :].astype(BF16) + accu[k, :].astype(BF16)).astype(F32)
            wide = h1[k, :].astype(F32)
            by = scale[k, :1]
            by_scale = jnp.sum(by_a * wide, -1, keepdims=True)
            by_wide = by_a * by + wide * (by_scale * (by * by * by) * (-1.0 / 512))
            dh[k, :] = dy[k, :] + by_wide.astype(BF16)


def weight_gradients(at, yt, s, dg, du, og, ou, od):
    for half in range(2):
        rows = slice(half * 256, half * 256 + 256)
        og[half * 8 : half * 8 + 8, 0] = dot(at[rows, :], dg[...]).astype(BF16).reshape(8, 32, TILE)
        ou[half * 8 : half * 8 + 8, 0] = dot(at[rows, :], du[...]).astype(BF16).reshape(8, 32, TILE)
        od[:, rows] = dot(yt[rows, :], s[...]).astype(BF16).T


def first_kernel(x, dy, wd, gate, up, og, ou, od, a, at, yt, s, dg, du, ds):
    j = pl.program_id(0)

    @pl.when(j == 0)
    def _():
        norm_into(x, a)
        flip_into(a, at)
        flip_into(dy, yt)

    for r in range(0, ROWS, CHUNK):
        rows = pl.ds(r, CHUNK)
        ds[rows, :] = dot(dy[rows, :], wd[0], ((1,), (1,)))
        for i in range(r, r + CHUNK, PIECE):
            k = slice(i, i + PIECE)
            s[k, :], dg[k, :], du[k, :] = gated(gate[k, :], up[k, :], ds[k, :])
    weight_gradients(at, yt, s, dg, du, og, ou, od)


def terms(x, dy, w_gate, w_up, w_down):
    vmem = pltpu.VMEM
    steps = 4096 // TILE
    full = pl.BlockSpec((ROWS, 512), lambda j: (0, 0))
    tile = pl.BlockSpec((ROWS, TILE), lambda j: (0, j))
    shape = jax.ShapeDtypeStruct
    states, wide = shape((ROWS, 512), BF16), shape((ROWS, 4096), F32)

    def weight(l):
        return [pl.BlockSpec((1, 512, TILE), lambda j: (l, 0, j))] * 2 + [pl.BlockSpec((1, TILE, 512), lambda j: (l, j, 0))]

    grads = [shape((16, 8, 32, TILE), BF16)] * 2 + [shape((4096, 512), BF16)]
    grad_specs = [pl.BlockSpec((16, 1, 32, TILE), lambda j: (0, j, 0, 0))] * 2 + [pl.BlockSpec((TILE, 512), lambda j: (j, 0))]
    b, t, f = vmem((ROWS, 512), BF16), vmem((512, ROWS), BF16), vmem((ROWS, 512), F32)
    o = vmem((512, TILE), F32)

    def call(kernel, dots, name, out_shape, in_specs, out_specs, scratch, *args):
        return pl.pallas_call(
            kernel, out_shape=out_shape, grid=(steps,), in_specs=in_specs, out_specs=out_specs, scratch_shapes=scratch, name=name,
            compiler_params=pltpu.CompilerParams(dimension_semantics=("arbitrary",), vmem_limit_bytes=60 * 2**20),
            cost_estimate=pl.CostEstimate(flops=dots * 2 * 1024 * 512 * 4096, bytes_accessed=30 * 2**20, transcendentals=2**22),
        )(*args)

    gate, up, h1 = call(forward_kernel, 3, "forward", [wide, wide, states], [full] + weight(0), [tile, tile, full], [b, b, f], x, w_gate, w_up, w_down)
    g1 = call(last_kernel, 8, "last", grads + [states], [full, full] + weight(1), grad_specs + [full],
              [b, t, t, b, b, b, o, o, o, f, f, f, f, f, vmem((ROWS, 128), F32)], h1, dy, w_gate, w_up, w_down)
    *g1, dh = g1
    g0 = call(first_kernel, 4, "first", grads, [full, full, weight(0)[2], tile, tile], grad_specs, [b, t, t, b, b, b, f], x, dh, w_down, gate, up)
    return [[g[c].reshape(4096, 512) for g in (g0, g1)] for c in range(3)]


def place():
    me = lax.axis_index("dp")
    return me, lax.rem(me, 2), [lax.rem(lax.div(me, s), 4) for s in STRIDE]


def neighbour(me, p, d, by):
    return me + (lax.rem(p[d] + by, 4) - p[d]) * STRIDE[d]


HALF, SIZES = 2048, (512, 128, 32)


def reduce_kernel(g00, g01, g10, g11, g20, g21, c0, c1, c2, factor, H, R0, R1, R2, R3, F1, F2, C, N, sq,
                  lsem, ds, dr, ps, pr, gs, gr, ns, nr, osem):
    g, outs = ((g00, g01), (g10, g11), (g20, g21)), (c0, c1, c2)
    me, core, p = place()
    partner = me + 1 - 2 * core
    dims = [(c, (c + 1) % 3, (c + 2) % 3) for c in range(3)]

    def send(src, dst, s, r, to):
        copy = pltpu.make_async_remote_copy(src_ref=src, dst_ref=dst, send_sem=s, recv_sem=r, device_id={"dp": to}, device_id_type=pl.DeviceIdType.MESH)
        copy.start()
        return copy

    barrier = pltpu.get_barrier_semaphore()
    others = [partner] + [neighbour(me, p, d, by) for d in range(3) for by in (1, 2, 3)]
    for other in others:
        pl.semaphore_signal(barrier, inc=1, device_id={"dp": other}, device_id_type=pl.DeviceIdType.MESH)

    loads = [pltpu.make_async_copy(g[c][l].at[pl.ds(pl.multiple_of(core * HALF, HALF), HALF)], H.at[c, l], lsem.at[c, l]) for c in range(3) for l in range(2)]
    for l in (1, 0):
        for c in range(3):
            loads[2 * c + l].start()
    pl.semaphore_wait(barrier, len(others))

    swaps = {}
    for l in (1, 0):
        for by in (2, 3, 1, 0):
            for c in range(3):
                at = pl.multiple_of(lax.rem(p[c] + by, 4) * 512, 512)
                swaps[c, by, l] = send(g[c][l].at[pl.ds(pl.multiple_of((1 - core) * HALF, HALF) + at, 512)], R0.at[c, l, pl.ds(at, 512)], ds.at[c, by, l], dr.at[c, by, l], partner)

    sends = []
    received = (R1, R2, R3)

    def term(k, c, l, at, row, step):
        rows = pl.ds(pl.multiple_of(at + row, 16), step)
        if k == 0:
            return H[c, l, rows].astype(F32) + R0[c, l, rows].astype(F32)
        return (F1, F2)[k - 1][c, l, rows]

    def make(k, c, l, at, slots, keep):
        half = SIZES[k] // 2
        step = min(half, 32)

        def body(i, carry):
            row = pl.multiple_of(i * step, 16)
            total = term(k, c, l, at, row, step)
            for slot in slots:
                total += received[k][c, slot, l, pl.ds(row, step)].astype(F32)
            keep(row, step, total)
            return carry

        lax.fori_loop(0, half // step, body, 0)

    def leave(k, c, l, by, side, slots, to, slot):
        half = SIZES[k] // 2
        at = pl.multiple_of(lax.rem(p[dims[c][k]] + by, 4) * SIZES[k] + side * half, 16)
        base = pl.multiple_of(sum((p[dims[c][i]] * SIZES[i] for i in range(k)), at), 16)

        def keep(row, step, total):
            H[c, l, pl.ds(pl.multiple_of(base + row, 16), step)] = total.astype(BF16)

        make(k, c, l, at, slots, keep)
        sends.append(send(H.at[c, l, pl.ds(base, half)], received[k].at[c, slot, l], ps.at[k, c, slot, l], pr.at[k, c, slot, l], neighbour(me, p, dims[c][k], to)))

    def arrived(k, c, l, slot):
        here = received[k].at[c, slot, l]
        pltpu.make_async_copy(here, here, pr.at[k, c, slot, l]).wait()

    def far(k, l):
        for c in range(3):
            if k == 0:
                loads[2 * c + l].wait()
                swaps[c, 2, l].wait_recv()
            leave(k, c, l, 2, 0, (), 2 if k == 2 else 3, 0)
            leave(k, c, l, 2, 1, (), 2 if k == 2 else 1, 3)

    def near(k, l):
        for c in range(3):
            if k == 0:
                swaps[c, 3, l].wait_recv(), swaps[c, 1, l].wait_recv()
            leave(k, c, l, 3, 1, (), 3, 1)
            leave(k, c, l, 1, 0, (), 1, 4)
            if k == 2:
                leave(k, c, l, 3, 0, (), 3, 2)
                leave(k, c, l, 1, 1, (), 1, 5)

    def onward(k, l):
        for c in range(3):
            arrived(k, c, l, 0)
            leave(k, c, l, 3, 0, (0,), 3, 2)
            arrived(k, c, l, 3)
            leave(k, c, l, 1, 1, (3,), 1, 5)

    def mine(k, l):
        half = SIZES[k] // 2
        for c in range(3):
            if k == 0:
                swaps[c, 0, l].wait_recv()
            for slot in (1, 4, 2, 5, 0, 3) if k == 2 else (1, 4, 2, 5):
                arrived(k, c, l, slot)
            for side, slots in ((0, (2, 4, 0)), (1, (1, 5, 3))) if k == 2 else ((0, (2, 4)), (1, (1, 5))):
                at = pl.multiple_of(p[dims[c][k]] * SIZES[k] + side * half, 16)

                def keep(row, step, total):
                    if k < 2:
                        (F1, F2)[k][c, l, pl.ds(pl.multiple_of(side * half + row, 16), step)] = total
                    else:
                        rounded = total.astype(BF16)
                        C[c, l, pl.ds(pl.multiple_of(p[dims[c][1]] * 128 + p[dims[c][2]] * 32 + side * half, 16), step)] = rounded
                        wide = rounded.astype(F32)
                        wide = wide * wide
                        sq[...] += sum(wide[8 * a : 8 * a + 8, 128 * b : 128 * b + 128] for a in range(step // 8) for b in range(4))

                make(k, c, l, at, slots, keep)

    def square(n):
        to = [partner] if n == 0 else [neighbour(me, p, n - 1, by) for by in (1, 2, 3)]
        own = core if n == 0 else p[n - 1]
        N[n, own] = sq[...]
        return [send(sq, N.at[n, own], ns.at[n, i], nr.at[n, i], dev) for i, dev in enumerate(to)]

    def squared(n, copies):
        for copy in copies:
            copy.wait()
        sq[...] = N[n, 0] + N[n, 1] if n == 0 else (N[n, 0] + N[n, 1]) + (N[n, 2] + N[n, 3])

    def rows(c, k, by, side=None):
        at = lax.rem(p[dims[c][k]] + by, 4) * SIZES[k] + (p[dims[c][1]] * 128 if k == 2 else 0)
        if side is None:
            return pl.ds(pl.multiple_of(at, 32), SIZES[k])
        return pl.ds(pl.multiple_of(at + side * (SIZES[k] // 2), 16), SIZES[k] // 2)

    def spread(k, l):
        for c in range(3):
            own = C.at[c, l, rows(c, k, 0)]
            for i, to in ((0, 3), (1, 1), (2, 2)) if k == 2 else ((0, 3), (1, 1)):
                sends.append(send(own, own, gs.at[k - 1, c, i, l], gr.at[k - 1, c, i, l], neighbour(me, p, dims[c][k], to)))

    def relay(k, l):
        for c in range(3):
            for i, by, to in ((0, 1, 3), (1, 3, 1)):
                whole = C.at[c, l, rows(c, k, by)]
                pltpu.make_async_copy(whole, whole, gr.at[k - 1, c, i, l]).wait()
                part = C.at[c, l, rows(c, k, by, i)]
                sends.append(send(part, part, gs.at[k - 1, c, 2 + i, l], gr.at[k - 1, c, 2 + i, l], neighbour(me, p, dims[c][k], to)))

    def gathered(k, l):
        for c in range(3):
            if k == 2:
                for i, by in ((0, 1), (1, 3), (2, 2)):
                    whole = C.at[c, l, rows(c, k, by)]
                    pltpu.make_async_copy(whole, whole, gr.at[k - 1, c, i, l]).wait()
                continue
            for i in range(2):
                part = C.at[c, l, rows(c, k, 2, i)]
                pltpu.make_async_copy(part, part, gr.at[k - 1, c, 2 + i, l]).wait()

    stores = []

    def store(l):
        for c in range(3):
            stores.append(pltpu.make_async_copy(C.at[c, l], outs[c].at[l], osem.at[c, l]))
            stores[-1].start()

    sq[...] = jnp.zeros_like(sq)
    far(0, 1), near(0, 1), onward(0, 1)
    far(0, 0), near(0, 0)
    mine(0, 1), far(1, 1), near(1, 1)
    onward(0, 0)
    onward(1, 1)
    mine(1, 1), far(2, 1), near(2, 1)
    mine(0, 0), far(1, 0), near(1, 0)
    onward(1, 0)
    mine(2, 1), spread(2, 1)
    mine(1, 0), far(2, 0), near(2, 0)
    gathered(2, 1), spread(1, 1)
    mine(2, 0)
    copies = square(0)
    spread(2, 0)
    squared(0, copies)
    copies = square(1)
    gathered(2, 0), spread(1, 0)
    relay(1, 1)
    squared(1, copies)
    copies = square(2)
    gathered(1, 1), store(1)
    squared(2, copies)
    copies = square(3)
    relay(1, 0)
    squared(3, copies)
    factor[...] = jnp.full(factor.shape, jnp.minimum(1.0, 0.5 * lax.rsqrt(jnp.sum(sq[...], keepdims=True) / COUNT + 1e-30)), F32)
    gathered(1, 0), store(0)
    for copy in list(swaps.values()) + sends:
        copy.wait_send()
    for copy in stores:
        copy.wait()


def reduce_all(g):
    dma, vmem = pltpu.SemaphoreType.DMA, pltpu.VMEM
    hbm = pl.BlockSpec(memory_space=pl.ANY)
    return pl.pallas_call(
        reduce_kernel,
        out_shape=[jax.ShapeDtypeStruct((2, 512, 512), BF16)] * 3 + [jax.ShapeDtypeStruct((8, 128), F32)],
        in_specs=[hbm] * 6,
        out_specs=[hbm] * 3 + [pl.BlockSpec(memory_space=pltpu.VMEM)],
        scratch_shapes=[
            vmem((3, 2, HALF, 512), BF16),
            vmem((3, 2, HALF, 512), BF16),
            vmem((3, 6, 2, 256, 512), BF16),
            vmem((3, 6, 2, 64, 512), BF16),
            vmem((3, 6, 2, 16, 512), BF16),
            vmem((3, 2, 512, 512), F32),
            vmem((3, 2, 128, 512), F32),
            vmem((3, 2, 512, 512), BF16),
            vmem((4, 4, 8, 128), F32),
            vmem((8, 128), F32),
            dma((3, 2)),
            dma((3, 4, 2)), dma((3, 4, 2)),
            dma((3, 3, 6, 2)), dma((3, 3, 6, 2)),
            dma((2, 3, 4, 2)), dma((2, 3, 4, 2)),
            dma((4, 3)), dma((4, 3)),
            dma((3, 2)),
        ],
        compiler_params=pltpu.CompilerParams(collective_id=1, has_side_effects=True, vmem_limit_bytes=60 * 2**20),
        name="reduce_all",
    )(*g)


def adamw_kernel(n_g, first, start, meta, f, *refs):
    unit = pl.program_id(0)
    ins, refs = refs[:9], refs[9:]
    g, refs = refs[: 3 * n_g], refs[3 * n_g :]
    outs = refs if first else refs[9:]
    outs[9][...] = jnp.zeros_like(outs[9])
    factor = f[0, 0]

    def update(c, gref):
        w, m, v = ins[c], ins[3 + c], ins[6 + c]
        ow, om, ov = outs[c], outs[3 + c], outs[6 + c]
        for half in range(2):
            def body(i, carry):
                if c < 2:
                    at = (0, pl.ds(half * 32, 32), pl.ds(pl.multiple_of(i * 512, 512), 512))
                else:
                    at = (0, pl.ds(pl.multiple_of(half * 256 + i * 32, 32), 32), slice(None))
                wide = gref[0, half * 8 + i].astype(F32) * factor
                nm = 0.9 * m[at] + 0.1 * wide
                nv = 0.95 * v[at] + 0.05 * wide * wide
                old = w[at].astype(F32)
                om[at] = nm
                ov[at] = nv
                ow[at] = (old - 0.02 * (nm * lax.rsqrt(nv + 1e-8) + 0.1 * old)).astype(BF16)
                return carry

            lax.fori_loop(0, 8, body, 0, unroll=2)

    for k in range(n_g):
        @pl.when(unit == k)
        def _():
            for c in range(3):
                update(c, g[3 * k + c])


def adamw_part(meta, start, units, f, state, so_far):
    n_g = len(units)

    def rows(c):
        return lambda u, meta: (meta[start + u, 3], meta[start + u, c], 0)

    wide, tall = (1, 64, 4096), (1, 512, 512)
    state_specs = [pl.BlockSpec(tall if c == 2 else wide, rows(c)) for _ in range(3) for c in range(3)]
    grads, grad_specs = [], []
    for arrays, index in units:
        for c in range(3):
            grads.append(arrays[c].reshape(arrays[c].shape[0], 16, 32, 512))
            grad_specs.append(pl.BlockSpec((1, 16, 32, 512), lambda u, meta, index=index: (index, 0, 0, 0)))
    before = [] if so_far is None else list(so_far)
    shapes = [jax.ShapeDtypeStruct(a.shape, a.dtype) for a in state] + [jax.ShapeDtypeStruct((8, 128), F32)]
    elements = n_g * 3 * 262144
    return pl.pallas_call(
        functools.partial(adamw_kernel, n_g, so_far is None, start),
        out_shape=shapes,
        grid_spec=pltpu.PrefetchScalarGridSpec(
            num_scalar_prefetch=1,
            grid=(n_g,),
            in_specs=[pl.BlockSpec((8, 128), lambda u, meta: (0, 0), memory_space=pltpu.SMEM)] + state_specs + grad_specs + [pl.BlockSpec(memory_space=pl.ANY)] * len(before),
            out_specs=state_specs + [pl.BlockSpec((8, 128), lambda u, meta: (0, 0))],
        ),
        input_output_aliases={2 + 9 + 3 * n_g + i: i for i in range(len(before))},
        compiler_params=pltpu.CompilerParams(dimension_semantics=("arbitrary",), vmem_limit_bytes=62 * 2**20),
        cost_estimate=pl.CostEstimate(flops=elements * 400, bytes_accessed=elements * 22, transcendentals=elements),
        name="adamw",
    )(meta, f, *state, *grads, *before)


def ring(d, by):
    return [(i, i + ((i // STRIDE[d] % 4 + by) % 4 - i // STRIDE[d] % 4) * STRIDE[d]) for i in range(128)]


PARTNER = [(i, i ^ 1) for i in range(128)]


def finish(g, weights, m, v):
    c0, c1, c2, f = reduce_all([g[c][l] for c in range(3) for l in range(2)])
    own = (c0, c1, c2)

    def swap(arrays):
        return [lax.ppermute(a, "dp", PARTNER) for a in arrays]

    after = [lax.ppermute(own[c], "dp", ring(c, 3)) for c in range(3)]
    ahead = [lax.ppermute(own[c], "dp", ring(c, 1)) for c in range(3)]
    own_x = swap(own)

    me, core, p = place()
    order = [(0, 0), (0, 1), (1, 0), (3, 0), (1, 1), (3, 1), (2, 0), (2, 1)]
    flip = jnp.array([other for _, other in order], jnp.int32)
    by = jnp.array([by for by, _ in order], jnp.int32)
    first = (core ^ flip) * 4
    meta = jnp.stack([first + lax.rem(p[c] + by, 4) for c in range(3)], -1)
    meta = jnp.concatenate([jnp.repeat(meta, 2, 0), jnp.array([[l] for _ in order for l in range(2)], jnp.int32)], -1)

    def both(*sets):
        return [(arrays, l) for arrays in sets for l in range(2)]

    def held(arrays, token):
        return [lax.optimization_barrier((a, token))[0] for a in arrays]

    state = [*weights, *m, *v]
    *so_far, token = adamw_part(meta, 0, both(own), f, state, None)
    *so_far, token = adamw_part(meta, 2, both(own_x), f, state, so_far)
    after_held, ahead_held = held(after, token), held(ahead, token)
    far = [lax.ppermute(after_held[c], "dp", ring(c, 3)) for c in range(3)]
    after_x, ahead_x = swap(after_held), swap(ahead_held)
    *so_far, token = adamw_part(meta, 4, both(after, ahead), f, state, so_far)
    far_x = swap(held(far, token))
    *so_far, token = adamw_part(meta, 8, both(after_x, ahead_x, far), f, state, so_far)
    *so_far, token = adamw_part(meta, 14, both(far_x), f, state, so_far)
    return tuple(so_far)


def solution(mesh):
    def step(x, dy, *arrays):
        weights, m, v = (arrays[i : i + 3] for i in (0, 3, 6))
        return finish(terms(x[0], dy[0], *weights), weights, m, v)

    return jax.shard_map(
        step,
        mesh=mesh,
        in_specs=(P(("rep", "dp"), None, None),) * 2 + (P(None, None, None),) * 9,
        out_specs=(P("rep", None, None),) * 9,
        check_vma=False,
    )
```
